32 devices in a mesh: groups: 2 (over y), fft: 4 (over z), band: 2 (over x), sub: 2 (over core).
Axes of the slice: x: 2, y: 2, z: 4, core: 2. Of those that a mesh axis runs over, the one named last changes fastest.
Arguments:
- coefficients: bfloat16 [8, 2, 128, 1024], P(('groups', 'band', 'sub'), None, None, 'fft'), parts along dimension 0, may hold values from -6 to 6
- potential: float32 [384, 192, 192], P(('groups', 'fft')), parts along dimension 0, may hold values from -15 to 15
- stick_map: int32 [3, 2048], P(None, ('groups', 'fft')), parts along dimension 1, may hold values from 0 to 191, as said below
- plane_order: int32 [384], P('groups'), parts along dimension 0, may hold values from 0 to 191, each once
Outputs:
- applied: float32 [8, 2, 128, 1024], P(('groups', 'band', 'sub'), None, None, 'fft'), parts along dimension 0
The draws below stay inside these ranges and needn't reach their ends.
There are 2 independent parts, one for each index of `groups`. The reference program is written for one: setup_inputs(seed, part) draws one part's arguments, and reference() takes and returns one part's arrays. A program takes and returns all parts, laid end to end along the dimension named above; each array names one. Nothing has to cross between parts.
Inputs may be any that keep to these rules, and one draw needn't show every extreme that they name: Column s is one stick slot: stick_map[0, s] and stick_map[1, s] are its grid indices x and y, stick_map[2, s] its length, an odd number up to 127, or 0 for an empty slot. A stick of length L holds the frequencies -(L - 1)/2 to (L - 1)/2 at entries 128/2 + f. The number of live slots differs between indices of fft; some index has all 256 slots live, and 512 slots are live in all. Live sticks name distinct columns, whose frequencies (indices taken modulo 192 into -96 to 95) lie in -48 to 47 along x and along y; an empty slot may name any column. `plane_order`: each plane number appears once.
All inputs are finite; a program needn't handle non-finite values.
Results may differ from the reference program's by a relative error of at most 0.0084.
Values may be sent and summed in bfloat16 or wider, within the bound.
No kernel may reach another device: no remote copies, remote signals or barrier semaphores. Data moves between devices by JAX's collectives and lax.ppermute only.
A program may use at most 128 MiB of HBM per device.

```python
import math
import jax
import jax.numpy as jnp
from jax import lax

N = 192
ZSPAN = 128
ST_DEV = 128
SLOTS = 256
STICKS = 512
WIN = 48
BANDS = 4
N_FFT = 4


def draw_stick_map(key, part):
    devices = STICKS // ST_DEV
    side_len = 2 * WIN
    cell_ids = jax.random.permutation(jax.random.fold_in(key, 101), side_len * side_len)[:STICKS]
    freq_x = cell_ids // side_len - WIN
    freq_y = cell_ids % side_len - WIN
    radius_sq = freq_x * freq_x + freq_y * freq_y
    z_steps = jnp.arange(1, ZSPAN // 2, dtype=jnp.int32)
    inside = radius_sq[:, None] + z_steps[None, :] * z_steps[None, :] <= 2 * WIN * WIN
    half_len = jnp.sum(inside.astype(jnp.int32), axis=1)
    lengths = 2 * half_len + 1
    dev_order = jax.random.permutation(jax.random.fold_in(key, 202), devices)
    dev_rank = jnp.argsort(dev_order)
    others = devices - 1
    positions = jnp.arange(devices, dtype=jnp.int32)
    removal = ST_DEV * 2 * positions // (others * (others + 1))
    leftover = ST_DEV - jnp.sum(removal)
    removal = removal + jnp.where(positions == others, leftover, 0)
    by_rank = jnp.where(positions == 0, SLOTS, ST_DEV - removal)
    counts = by_rank[dev_rank]
    offsets = jnp.cumsum(counts) - counts
    slot_keys = jax.random.split(jax.random.fold_in(key, 303), devices)
    slot_rank = jax.vmap(lambda one_key: jax.random.permutation(one_key, SLOTS))(slot_keys)
    is_live = slot_rank < counts[:, None]
    stick_id = jnp.minimum(offsets[:, None] + slot_rank, STICKS - 1)
    pos_x = freq_x[stick_id] % N
    pos_y = freq_y[stick_id] % N
    live_len = jnp.where(is_live, lengths[stick_id], 0)
    return jnp.stack([pos_x.reshape(-1), pos_y.reshape(-1), live_len.reshape(-1)], 0).astype(jnp.int32)


def steps_of(key, dims, pieces, low, top_value):
    level, own = 1.0, jax.random.fold_in(key, 6)
    for position, shards_of in pieces:
        steps = jnp.exp(jax.random.uniform(jax.random.fold_in(own, position), (shards_of,), jnp.float32, low / len(pieces), top_value / len(pieces)))
        level = level * jnp.repeat(steps, dims[position] // shards_of).reshape([-1 if axis == position else 1 for axis in range(len(dims))])
    return level


def noise(rng, shape, scale, reach, shards=(), kind=jnp.bfloat16):
    values = jax.random.normal(rng, shape, jnp.float32) * scale
    if len(shards) > 0:
        values = steps_of(rng, shape, shards, -0.22, 0.18) * values
    return jnp.clip(values, min=-reach, max=reach).astype(kind)


def setup_inputs(seed: int = 0, part: int = 0) -> dict:
    streams_of = jax.random.split(jax.random.key(seed), 5)
    part_splits = jax.random.split(jax.random.fold_in(streams_of[4], part), 5)
    return {
        "coefficients": noise(part_splits[0], (BANDS, 2, ZSPAN, N_FFT * SLOTS), 1.0, 6.0, ((0, 4), (3, 4))),
        "potential": noise(part_splits[1], (N, N, N), 3.0, 15.0, ((0, 4),), jnp.float32),
        "stick_map": draw_stick_map(jax.random.fold_in(jax.random.fold_in(streams_of[4], part), 71), part),
        "plane_order": jax.random.permutation(part_splits[3], N).astype(jnp.int32),
    }


def phase_tables(left_ids, right_ids, modulus):
    turn_index = (left_ids[:, None] * right_ids[None, :]) % modulus
    angles = turn_index.astype(jnp.float32) * (2.0 * math.pi / modulus)
    return jnp.cos(angles).astype(jnp.bfloat16), jnp.sin(angles).astype(jnp.bfloat16)


def as_wide(values):
    return values.astype(jnp.float32)


def reference(coefficients, potential, stick_map, plane_order):
    z_span = coefficients.shape[2]
    slot_total = coefficients.shape[3]
    grid_side = potential.shape[1]
    entries = jnp.arange(z_span, dtype=jnp.int32)
    freq_z = (entries - z_span // 2) % grid_side
    half_len = (stick_map[2] - 1) // 2
    keep_mask = jnp.abs(entries[:, None] - z_span // 2) <= half_len[None, :]
    keep_low = keep_mask.astype(jnp.bfloat16)
    keep_wide = keep_mask.astype(jnp.float32)
    cos_z, sin_z = phase_tables(plane_order, freq_z, grid_side)
    forward_z = jnp.stack([jnp.concatenate([cos_z, -sin_z], 1), jnp.concatenate([sin_z, cos_z], 1)], 1)
    inverse_z = jnp.stack([jnp.stack([cos_z, sin_z], 1), jnp.stack([-sin_z, cos_z], 1)], 1)
    axis_ids = jnp.arange(grid_side, dtype=jnp.int32)
    cos_g, sin_g = phase_tables(axis_ids, axis_ids, grid_side)
    forward_y = jnp.concatenate([jnp.concatenate([cos_g, sin_g], 1), jnp.concatenate([-sin_g, cos_g], 1)], 0)
    inverse_y = jnp.concatenate([jnp.concatenate([cos_g, -sin_g], 1), jnp.concatenate([sin_g, cos_g], 1)], 0)
    both_x = jnp.concatenate([cos_g, sin_g], 0)
    comp_ids = jnp.arange(2, dtype=jnp.int32)
    flat_ids = (stick_map[0][None, :] * (2 * grid_side) + comp_ids[:, None] * grid_side + stick_map[1][None, :]).reshape(-1)
    scale = 1.0 / grid_side ** 3

    def one_band(coeff_band):
        masked = (coeff_band * keep_low).reshape(2 * z_span, slot_total)
        sticks = jnp.einsum("zck,ks->zcs", as_wide(forward_z), as_wide(masked)).astype(jnp.bfloat16)
        blank_grid = jnp.zeros((grid_side, 2 * grid_side * grid_side), jnp.bfloat16)
        spread = blank_grid.at[:, flat_ids].add(sticks.reshape(grid_side, 2 * slot_total))
        half_y = jnp.dot(as_wide(spread.reshape(-1, 2 * grid_side)), as_wide(forward_y), preferred_element_type=jnp.float32)
        half_y = half_y.astype(jnp.bfloat16).reshape(grid_side, grid_side, 2 * grid_side)
        mixed_x = jnp.einsum("ux,rxw->ruw", as_wide(both_x), as_wide(half_y))
        cos_part = mixed_x[:, :grid_side]
        sin_part = mixed_x[:, grid_side:]
        real_part = (cos_part[..., :grid_side] - sin_part[..., grid_side:]) * potential
        imag_part = (cos_part[..., grid_side:] + sin_part[..., :grid_side]) * potential
        product = jnp.concatenate([real_part, imag_part], 2).astype(jnp.bfloat16)
        mixed_x = jnp.einsum("ux,rxw->ruw", as_wide(both_x), as_wide(product))
        cos_part = mixed_x[:, :grid_side]
        sin_part = mixed_x[:, grid_side:]
        back_x = jnp.concatenate([cos_part[..., :grid_side] + sin_part[..., grid_side:], cos_part[..., grid_side:] - sin_part[..., :grid_side]], 2).astype(jnp.bfloat16)
        back_y = jnp.dot(as_wide(back_x.reshape(-1, 2 * grid_side)), as_wide(inverse_y), preferred_element_type=jnp.float32).astype(jnp.bfloat16)
        columns = jnp.take(back_y.reshape(grid_side, -1), flat_ids, axis=1).reshape(grid_side, 2, slot_total)
        totals = jnp.einsum("rcdk,rds->cks", as_wide(inverse_z), as_wide(columns))
        return totals * (keep_wide * scale)

    return lax.map(one_band, coefficients)
```

```python
import functools
import math

import jax
import jax.numpy as jnp
import numpy as np
from jax import lax
from jax.experimental import pallas as pl
from jax.experimental.pallas import tpu as pltpu
from jax.sharding import PartitionSpec as P

F32 = jnp.float32
BF16 = jnp.bfloat16


def angle_tables(left_ids, right_ids, modulus):
    turns = (left_ids[:, None] * right_ids[None, :]) % modulus
    angles = turns * (2.0 * math.pi / modulus)
    return np.cos(angles), np.sin(angles)


def pad_to(array, rows, cols):
    return np.pad(array, ((0, rows - array.shape[0]), (0, cols - array.shape[1])))


def z_constants(grid_side, z_span):
    planes = np.arange(grid_side)
    freq = (np.arange(z_span) - z_span // 2) % grid_side
    cos_z, sin_z = angle_tables(planes, freq, grid_side)
    forward = np.concatenate([cos_z, -sin_z, sin_z, cos_z], 1)
    inverse = np.concatenate([cos_z.T, sin_z.T], 0)
    return jnp.asarray(forward, BF16), jnp.asarray(inverse, BF16)


def axis_constants(grid_side, lane_pad):
    half = grid_side // 2
    quarter = half // 2
    grid_ids = np.arange(grid_side)
    compact = np.arange(half)
    window = np.where(compact < quarter, compact, compact + half)
    cos_w, sin_w = angle_tables(window, grid_ids, grid_side)

    def by_high(top, bottom):
        parts = []
        for high in range(2):
            rows = slice(high * quarter, (high + 1) * quarter)
            parts += [top[rows], bottom[rows]]
        return np.concatenate(parts, 0)

    forward_x = np.concatenate([by_high(cos_w, -sin_w).T, by_high(sin_w, cos_w).T], 0)
    pad = functools.partial(pad_to, rows=lane_pad, cols=grid_side)
    forward_y = np.stack(
        [
            np.concatenate([pad(cos_w), pad(-sin_w)], 0),
            np.concatenate([pad(sin_w), pad(cos_w)], 0),
        ]
    )
    inverse_y = np.stack(
        [
            np.concatenate([pad(cos_w).T, pad(-sin_w).T], 1),
            np.concatenate([pad(sin_w).T, pad(cos_w).T], 1),
        ]
    )
    inverse_x = np.stack([by_high(cos_w, -sin_w), by_high(sin_w, cos_w)])
    return tuple(jnp.asarray(t, BF16) for t in (forward_x, forward_y, inverse_y, inverse_x))


def mm(left, right):
    return jnp.dot(left, right, preferred_element_type=F32)


def mm_t(left, right):
    return lax.dot_general(left, right, (((0,), (0,)), ((), ())), preferred_element_type=F32)


def stick_kernel(coeff, smap, order, fwd, inv, out, table, *, owners, share):
    bands, _, z_span, slots = coeff.shape
    grid_side = order.shape[1]
    chosen = lax.broadcasted_iota(jnp.int32, (grid_side, grid_side), 0) == order[...]
    chosen = chosen.astype(BF16)
    rows = mm_t(chosen, fwd[...]).astype(BF16)
    table[...] = mm(inv[...], chosen).astype(BF16)
    entries = lax.broadcasted_iota(jnp.int32, (z_span, slots), 0)
    half_len = (smap[2:3, :] + 1) // 2 - 1
    keep = jnp.abs(entries - z_span // 2) <= half_len
    for band in range(bands):
        parts = []
        for comp in range(2):
            values = coeff[band, comp].astype(F32)
            parts.append(jnp.where(keep, values, 0.0).astype(BF16))
        masked = jnp.concatenate(parts, 0)
        for comp in range(2):
            sticks = mm(rows[:, comp * 2 * z_span : (comp + 1) * 2 * z_span], masked).astype(BF16)
            col = (band * 2 + comp) * slots
            for owner in range(owners):
                out[owner, 0:share, col : col + slots] = sticks[owner * share : (owner + 1) * share]
    spare = out.shape[1] - share
    places = jnp.concatenate([smap[0:1, :], smap[1:2, :]], 1).astype(F32)
    places = jnp.broadcast_to(places, (spare, 2 * slots)).astype(BF16)
    for owner in range(owners):
        out[owner, share:, 0 : 2 * slots] = places
        if bands > 1:
            out[owner, share:, 2 * slots :] = jnp.zeros((spare, (bands - 1) * 2 * slots), BF16)


def plane_kernel(
    recv, pot, fwd_x, fwd_y, inv_y, inv_x, out, vals, low, high_t, high, acc, *, bands, slots, share, group
):
    sources = recv.shape[0]
    grid_side = pot.shape[1]
    half = grid_side // 2
    quarter = half // 2
    lane_pad = high.shape[0] // 2
    step = pl.program_id(0)

    @pl.when(step == 0)
    def _():
        for src in range(sources):
            cols = slice(src * slots, (src + 1) * slots)
            vals[src] = recv[src, 0:share, :].astype(F32)
            place = recv[src, share:, 0 : 2 * slots].astype(F32)[0:1].astype(jnp.int32)
            compact = jnp.where(place < quarter, place, place - half)
            compact = jnp.clip(compact, 0, half - 1)
            x_id = compact[:, 0:slots]
            y_id = compact[:, slots : 2 * slots]
            x_high = jnp.where(x_id >= quarter, 1, 0)
            x_low = x_id - x_high * quarter
            rows = lax.broadcasted_iota(jnp.int32, (quarter, slots), 0)
            low[:, cols] = jnp.where(rows == x_low, 1.0, 0.0)
            rows = lax.broadcasted_iota(jnp.int32, (2 * lane_pad, slots), 0)
            hot = jnp.where(rows == x_high * lane_pad + y_id, 1.0, 0.0)
            high[:, cols] = hot.astype(BF16)
            high_t[cols, :] = hot.T.astype(BF16)

    base = step * group
    units = [(plane, band) for plane in range(group) for band in range(bands)]
    pairs = [units[i : i + 2] for i in range(0, len(units), 2)]
    low_hot = low[...].astype(BF16)

    def spread(pair):
        stacked = []
        for plane, band in pair:
            for comp in range(2):
                col = (band * 2 + comp) * slots
                pieces = []
                for src in range(sources):
                    row = vals[src, pl.ds(base + plane, 1), col : col + slots]
                    row = jnp.broadcast_to(row, (quarter, slots)).astype(BF16)
                    pieces.append(row * low_hot[:, src * slots : (src + 1) * slots])
                stacked.append(jnp.concatenate(pieces, 1))
        spots = mm(jnp.concatenate(stacked, 0), high_t[...]).astype(BF16)
        lanes = []
        for i in range(len(pair)):
            rows = spots[i * half : (i + 1) * half]
            lanes.append(jnp.concatenate([rows[:, :lane_pad], rows[:, lane_pad:]], 0))
        return jnp.concatenate(lanes, 1)

    def along_x(grid):
        return mm(fwd_x[...], grid).astype(BF16)

    def along_y(grid):
        stacked = []
        for i in range(grid.shape[1] // lane_pad):
            cols = slice(i * lane_pad, (i + 1) * lane_pad)
            stacked.append(jnp.concatenate([grid[:grid_side, cols], grid[grid_side:, cols]], 1))
        stacked = jnp.concatenate(stacked, 0)
        return mm(stacked, fwd_y[0]), mm(stacked, fwd_y[1])

    def times_potential(pair, fields):
        real, imag = [], []
        for i, (plane, _) in enumerate(pair):
            rows = slice(i * grid_side, (i + 1) * grid_side)
            field = pot[plane]
            real.append((fields[0][rows] * field).astype(BF16))
            imag.append((fields[1][rows] * field).astype(BF16))
        return jnp.concatenate(real, 0), jnp.concatenate(imag, 0)

    def back_y(product):
        return (mm(product[0], inv_y[0]) + mm(product[1], inv_y[1])).astype(BF16)

    def back_x(grid):
        count = grid.shape[0] // grid_side
        total = None
        for comp in range(2):
            cols = slice(comp * lane_pad, (comp + 1) * lane_pad)
            rhs = [grid[i * grid_side : (i + 1) * grid_side, cols] for i in range(count)]
            part = mm(inv_x[comp], jnp.concatenate(rhs, 1))
            total = part if total is None else total + part
        return total.astype(BF16)

    def pick(pair, grid):
        stacked = []
        for i in range(len(pair)):
            cols = slice(i * lane_pad, (i + 1) * lane_pad)
            stacked.append(jnp.concatenate([grid[:half, cols], grid[half:, cols]], 1))
        found = mm(jnp.concatenate(stacked, 0), high[...])
        for i, (plane, band) in enumerate(pair):
            for comp in range(2):
                start = i * half + comp * quarter
                line = jnp.sum(found[start : start + quarter] * low[...], axis=0, keepdims=True)
                col = (band * 2 + comp) * slots
                for src in range(sources):
                    acc[src, pl.ds(base + plane, 1), col : col + slots] = line[
                        :, src * slots : (src + 1) * slots
                    ]

    grids = [spread(pair) for pair in pairs]
    grids = [along_x(grid) for grid in grids]
    fields = [along_y(grid) for grid in grids]
    products = [times_potential(pair, field) for pair, field in zip(pairs, fields)]
    grids = [back_y(product) for product in products]
    grids = [back_x(grid) for grid in grids]
    for pair, grid in zip(pairs, grids):
        pick(pair, grid)

    @pl.when(step == pl.num_programs(0) - 1)
    def _():
        for src in range(sources):
            out[src] = acc[src].astype(BF16)


def column_kernel(returned, smap, table, out, *, slots):
    bands, _, z_span, _ = out.shape
    grid_side = returned.shape[0]
    entries = lax.broadcasted_iota(jnp.int32, (z_span, slots), 0)
    half_len = (smap[2:3, :] + 1) // 2 - 1
    keep = jnp.abs(entries - z_span // 2) <= half_len
    scale = jnp.where(keep, 1.0 / grid_side**3, 0.0)
    for band in range(bands):
        real = returned[:, band * 2 * slots : (band * 2 + 1) * slots]
        imag = returned[:, (band * 2 + 1) * slots : (band * 2 + 2) * slots]
        by_real = mm(table[...], real)
        by_imag = mm(table[...], imag)
        out[band, 0] = (by_real[:z_span] + by_imag[z_span:]) * scale
        out[band, 1] = (by_imag[:z_span] - by_real[z_span:]) * scale


def body(coefficients, potential, stick_map, plane_order):
    bands, _, z_span, slots = coefficients.shape
    share, grid_side, _ = potential.shape
    owners = lax.axis_size("fft")
    width = bands * 2 * slots
    lane_pad = -(-(grid_side // 2) // 128) * 128
    rows_sent = (share // 8 + 1) * 8
    order = plane_order.reshape(1, grid_side)
    params = pltpu.CompilerParams(vmem_limit_bytes=48 << 20)

    fwd_z, inv_z = z_constants(grid_side, z_span)
    sent, table = pl.pallas_call(
        functools.partial(stick_kernel, owners=owners, share=share),
        out_shape=(
            jax.ShapeDtypeStruct((owners, rows_sent, width), BF16),
            jax.ShapeDtypeStruct((2 * z_span, grid_side), BF16),
        ),
        compiler_params=params,
        name="sticks",
    )(coefficients, stick_map, order, fwd_z, inv_z)

    received = lax.all_to_all(sent, "fft", split_axis=0, concat_axis=0, tiled=True)

    group = next(g for g in (4, 2, 1) if share % g == 0)
    tables = axis_constants(grid_side, lane_pad)

    def whole(shape):
        return pl.BlockSpec(shape, lambda i: (0,) * len(shape), pipeline_mode=pl.Buffered(1))

    total = owners * slots
    columns = pl.pallas_call(
        functools.partial(plane_kernel, bands=bands, slots=slots, share=share, group=group),
        grid=(share // group,),
        in_specs=[
            whole((owners, rows_sent, width)),
            pl.BlockSpec((group, grid_side, grid_side), lambda i: (i, 0, 0)),
        ]
        + [whole(t.shape) for t in tables],
        out_specs=whole((owners, share, width)),
        out_shape=jax.ShapeDtypeStruct((owners, share, width), BF16),
        scratch_shapes=[
            pltpu.VMEM((owners, share, width), F32),
            pltpu.VMEM((grid_side // 4, total), F32),
            pltpu.VMEM((total, 2 * lane_pad), BF16),
            pltpu.VMEM((2 * lane_pad, total), BF16),
            pltpu.VMEM((owners, share, width), F32),
        ],
        compiler_params=params,
        name="planes",
    )(received, potential, *tables)

    returned = lax.all_to_all(columns, "fft", split_axis=0, concat_axis=0, tiled=True)
    return pl.pallas_call(
        functools.partial(column_kernel, slots=slots),
        out_shape=jax.ShapeDtypeStruct(coefficients.shape, F32),
        compiler_params=params,
        name="columns",
    )(returned.reshape(grid_side, width), stick_map, table)


def solution(mesh):
    placed = (
        P(("groups", "band", "sub"), None, None, "fft"),
        P(("groups", "fft"), None, None),
        P(None, ("groups", "fft")),
        P("groups"),
    )
    return jax.shard_map(
        body,
        mesh=mesh,
        in_specs=placed,
        out_specs=P(("groups", "band", "sub"), None, None, "fft"),
        check_vma=False,
    )
```

```python
import functools
import math

import jax
import jax.numpy as jnp
import numpy as np
from jax import lax
from jax.experimental import pallas as pl
from jax.experimental.pallas import tpu as pltpu
from jax.sharding import PartitionSpec as P

F32 = jnp.float32
BF16 = jnp.bfloat16


def angle_tables(left_ids, right_ids, modulus):
    turns = (left_ids[:, None] * right_ids[None, :]) % modulus
    angles = turns * (2.0 * math.pi / modulus)
    return np.cos(angles), np.sin(angles)


def pad_to(array, rows, cols):
    return np.pad(array, ((0, rows - array.shape[0]), (0, cols - array.shape[1])))


def z_constants(grid_side, z_span):
    freq = (np.arange(z_span) - z_span // 2) % grid_side
    return jnp.asarray(np.concatenate(angle_tables(np.arange(grid_side), freq, grid_side), 1), BF16)


def axis_constants(grid_side, lane_pad):
    half = grid_side // 2
    quarter = half // 2
    grid_ids = np.arange(grid_side)
    compact = np.arange(half)
    window = np.where(compact < quarter, compact, compact + half)
    cos_w, sin_w = angle_tables(window, grid_ids, grid_side)

    def by_high(top, bottom):
        parts = []
        for high in range(2):
            rows = slice(high * quarter, (high + 1) * quarter)
            parts += [top[rows], bottom[rows]]
        return np.concatenate(parts, 0)

    forward_x = np.concatenate([by_high(cos_w, -sin_w).T, by_high(sin_w, cos_w).T], 0)
    pad = functools.partial(pad_to, rows=lane_pad, cols=grid_side)
    forward_y = np.stack(
        [
            np.concatenate([pad(cos_w), pad(-sin_w)], 0),
            np.concatenate([pad(sin_w), pad(cos_w)], 0),
        ]
    )
    inverse_y = np.stack(
        [
            np.concatenate([pad(cos_w).T, pad(-sin_w).T], 1),
            np.concatenate([pad(sin_w).T, pad(cos_w).T], 1),
        ]
    )
    inverse_x = np.stack([by_high(cos_w, -sin_w), by_high(sin_w, cos_w)])
    return tuple(jnp.asarray(t, BF16) for t in (forward_x, forward_y, inverse_y, inverse_x))


def mm(left, right):
    return jnp.dot(left, right, preferred_element_type=F32)


def mm_t(left, right):
    return lax.dot_general(left, right, (((0,), (0,)), ((), ())), preferred_element_type=F32)


def hops(owners):
    return (0,) + tuple(range(owners - 1, 0, -1))


def partner(index, hop, owners):
    return index ^ hop if owners & (owners - 1) == 0 else (index + hop) % owners


def copies_in(sources, targets, sems):
    started = [
        pltpu.make_async_copy(src, dst, sems.at[i]) for i, (src, dst) in enumerate(zip(sources, targets))
    ]
    for one in started:
        one.start()
    return started


def stick_kernel(me, coeff_h, smap_h, order_h, turn_h, *refs, owners, share):
    outs = refs[:owners]
    table, half_len, coeff, smap, order, turn, sticks, sems = refs[owners:]
    started = copies_in((order_h, turn_h, smap_h, coeff_h), (order, turn, smap, coeff), sems)
    bands, _, z_span, slots = coeff.shape
    grid_side = order.shape[1]
    started[0].wait()
    chosen = lax.broadcasted_iota(jnp.int32, (grid_side, grid_side), 0) == order[...]
    chosen = jnp.where(chosen, 1.0, 0.0).astype(BF16)
    started[1].wait()
    rows = mm_t(chosen, turn[...])
    table[...] = rows.T.astype(BF16)
    rows = rows.astype(BF16)
    cos_rows, sin_rows = rows[:, :z_span], rows[:, z_span:]
    lefts = (
        jnp.concatenate([cos_rows, -sin_rows], 1),
        jnp.concatenate([sin_rows, cos_rows], 1),
    )
    started[2].wait()
    entries = lax.broadcasted_iota(jnp.int32, (z_span, slots), 0)
    half = (smap[2:3, :] + 1) // 2 - 1
    half_len[...] = jnp.broadcast_to(half, half_len.shape)
    keep = jnp.abs(entries - z_span // 2) <= half
    started[3].wait()
    for band in range(bands):
        parts = []
        for comp in range(2):
            values = coeff[band, comp].astype(F32)
            parts.append(jnp.where(keep, values, 0.0).astype(BF16))
        masked = jnp.concatenate(parts, 0)
        for comp in range(2):
            found = mm(lefts[comp], masked).astype(BF16)
            col = (band * 2 + comp) * slots
            for owner in range(owners):
                sticks[owner, :, col : col + slots] = found[owner * share : (owner + 1) * share]
    spare = outs[0].shape[0] - share
    places = jnp.concatenate([smap[0:1, :], smap[1:2, :]], 1).astype(F32)
    places = jnp.broadcast_to(places, (spare, 2 * slots)).astype(BF16)
    for out, hop in zip(outs, hops(owners)):
        out[0:share, :] = sticks[partner(me[0], hop, owners)]
        out[share:, 0 : 2 * slots] = places
        if bands > 1:
            out[share:, 2 * slots :] = jnp.zeros((spare, (bands - 1) * 2 * slots), BF16)


def plane_kernel(*refs, sources, bands, slots, share, group):
    recv = refs[:sources]
    pot_h, *tables_h = refs[sources : sources + 5]
    outs = refs[sources + 5 : 2 * sources + 5]
    pot, fwd_x, fwd_y, inv_y, inv_x, vals, low, high_t, high, acc, table_sems, pot_sems = refs[2 * sources + 5 :]
    grid_side = pot.shape[1]
    half = grid_side // 2
    quarter = half // 2
    lane_pad = high.shape[0] // 2
    started = copies_in(tables_h, (fwd_x, fwd_y, inv_y, inv_x), table_sems)

    def pot_copy(step):
        rows = pl.ds(step * group, group)
        return pltpu.make_async_copy(pot_h.at[rows], pot.at[rows], pot_sems.at[step])

    for step in range(share // group):
        pot_copy(step).start()

    for src in range(sources):
        cols = slice(src * slots, (src + 1) * slots)
        vals[src] = recv[src][0:share, :].astype(F32)
        place = recv[src][share:, 0 : 2 * slots].astype(F32)[0:1].astype(jnp.int32)
        compact = jnp.where(place < quarter, place, place - half)
        compact = jnp.clip(compact, 0, half - 1)
        x_id = compact[:, 0:slots]
        y_id = compact[:, slots : 2 * slots]
        x_high = jnp.where(x_id >= quarter, 1, 0)
        x_low = x_id - x_high * quarter
        rows = lax.broadcasted_iota(jnp.int32, (quarter, slots), 0)
        low[:, cols] = jnp.where(rows == x_low, 1.0, 0.0)
        rows = lax.broadcasted_iota(jnp.int32, (2 * lane_pad, slots), 0)
        hot = jnp.where(rows == x_high * lane_pad + y_id, 1.0, 0.0)
        high[:, cols] = hot.astype(BF16)
        high_t[cols, :] = hot.T.astype(BF16)

    for one in started:
        one.wait()

    def one_group(step):
        base = step * group
        units = [(plane, band) for plane in range(group) for band in range(bands)]
        pairs = [units[i : i + 2] for i in range(0, len(units), 2)]
        low_hot = low[...].astype(BF16)

        def spread(pair):
            stacked = []
            for plane, band in pair:
                for comp in range(2):
                    col = (band * 2 + comp) * slots
                    pieces = []
                    for src in range(sources):
                        row = vals[src, pl.ds(base + plane, 1), col : col + slots]
                        row = jnp.broadcast_to(row, (quarter, slots)).astype(BF16)
                        pieces.append(row * low_hot[:, src * slots : (src + 1) * slots])
                    stacked.append(jnp.concatenate(pieces, 1))
            spots = mm(jnp.concatenate(stacked, 0), high_t[...]).astype(BF16)
            lanes = []
            for i in range(len(pair)):
                rows = spots[i * half : (i + 1) * half]
                lanes.append(jnp.concatenate([rows[:, :lane_pad], rows[:, lane_pad:]], 0))
            return jnp.concatenate(lanes, 1)

        def along_x(grid):
            return mm(fwd_x[...], grid).astype(BF16)

        def along_y(grid):
            stacked = []
            for i in range(grid.shape[1] // lane_pad):
                cols = slice(i * lane_pad, (i + 1) * lane_pad)
                stacked.append(jnp.concatenate([grid[:grid_side, cols], grid[grid_side:, cols]], 1))
            stacked = jnp.concatenate(stacked, 0)
            return mm(stacked, fwd_y[0]), mm(stacked, fwd_y[1])

        def times_potential(pair, fields):
            real, imag = [], []
            for i, (plane, _) in enumerate(pair):
                rows = slice(i * grid_side, (i + 1) * grid_side)
                field = pot[base + plane]
                real.append((fields[0][rows] * field).astype(BF16))
                imag.append((fields[1][rows] * field).astype(BF16))
            return jnp.concatenate(real, 0), jnp.concatenate(imag, 0)

        def back_y(product):
            return (mm(product[0], inv_y[0]) + mm(product[1], inv_y[1])).astype(BF16)

        def back_x(grid):
            count = grid.shape[0] // grid_side
            total = None
            for comp in range(2):
                cols = slice(comp * lane_pad, (comp + 1) * lane_pad)
                rhs = [grid[i * grid_side : (i + 1) * grid_side, cols] for i in range(count)]
                part = mm(inv_x[comp], jnp.concatenate(rhs, 1))
                total = part if total is None else total + part
            return total.astype(BF16)

        def pick(pair, grid):
            stacked = []
            for i in range(len(pair)):
                cols = slice(i * lane_pad, (i + 1) * lane_pad)
                stacked.append(jnp.concatenate([grid[:half, cols], grid[half:, cols]], 1))
            found = mm(jnp.concatenate(stacked, 0), high[...])
            for i, (plane, band) in enumerate(pair):
                for comp in range(2):
                    start = i * half + comp * quarter
                    line = jnp.sum(found[start : start + quarter] * low[...], axis=0, keepdims=True)
                    col = (band * 2 + comp) * slots
                    for src in range(sources):
                        acc[src, pl.ds(base + plane, 1), col : col + slots] = line[
                            :, src * slots : (src + 1) * slots
                        ]

        grids = [spread(pair) for pair in pairs]
        grids = [along_x(grid) for grid in grids]
        fields = [along_y(grid) for grid in grids]
        products = [times_potential(pair, field) for pair, field in zip(pairs, fields)]
        grids = [back_y(product) for product in products]
        grids = [back_x(grid) for grid in grids]
        for pair, grid in zip(pairs, grids):
            pick(pair, grid)

    @pl.loop(0, share // group)
    def _(step):
        pot_copy(step).wait()
        one_group(step)

    for src in range(sources):
        outs[src][...] = acc[src].astype(BF16)


def column_kernel(me, half_len, table, *refs, owners, slots):
    returned, (out, grid) = refs[:owners], refs[owners:]
    bands, _, z_span, _ = out.shape
    for part, hop in zip(returned, hops(owners)):
        grid[partner(me[0], hop, owners)] = part[...]
    entries = lax.broadcasted_iota(jnp.int32, (z_span, slots), 0)
    keep = jnp.abs(entries - z_span // 2) <= half_len[0:1, :]
    grid_side = table.shape[1]
    scale = jnp.where(keep, 1.0 / grid_side**3, 0.0)
    for band in range(bands):
        lines = []
        for comp in range(2):
            col = (band * 2 + comp) * slots
            lines.append(
                jnp.concatenate([grid[owner, :, col : col + slots] for owner in range(owners)], 0)
            )
        by_real = mm(table[...], lines[0])
        by_imag = mm(table[...], lines[1])
        out[band, 0] = (by_real[:z_span] + by_imag[z_span:]) * scale
        out[band, 1] = (by_imag[:z_span] - by_real[z_span:]) * scale


def exchange(parts, owners, back):
    result = [parts[0]]
    for part, hop in zip(parts[1:], hops(owners)[1:]):
        pairs = [(i, partner(i, hop, owners)) for i in range(owners)]
        if back:
            pairs = [(there, here) for here, there in pairs]
        with jax.named_scope(("back" if back else "send") + str(hop)):
            result.append(lax.ppermute(part, "fft", pairs))
    return result


def body(coefficients, potential, stick_map, plane_order):
    bands, _, z_span, slots = coefficients.shape
    share, grid_side, _ = potential.shape
    owners = lax.axis_size("fft")
    width = bands * 2 * slots
    lane_pad = -(-(grid_side // 2) // 128) * 128
    rows_sent = (share // 8 + 1) * 8
    params = pltpu.CompilerParams(vmem_limit_bytes=48 << 20)
    me = lax.axis_index("fft").astype(jnp.int32).reshape(1)
    in_smem = pl.BlockSpec(memory_space=pltpu.SMEM)
    in_hbm = pl.BlockSpec(memory_space=pltpu.HBM)
    in_vmem = pl.BlockSpec(memory_space=pltpu.VMEM)

    def stay(*arrays):
        return tuple(pltpu.with_memory_space_constraint(one, pltpu.HBM) for one in arrays)

    *sent, table, half_len = pl.pallas_call(
        functools.partial(stick_kernel, owners=owners, share=share),
        in_specs=[in_smem] + [in_hbm] * 4,
        out_shape=[jax.ShapeDtypeStruct((rows_sent, width), BF16)] * owners
        + [
            jax.ShapeDtypeStruct((2 * z_span, grid_side), BF16),
            jax.ShapeDtypeStruct((8, slots), jnp.int32),
        ],
        scratch_shapes=[
            pltpu.VMEM(coefficients.shape, BF16),
            pltpu.VMEM(stick_map.shape, jnp.int32),
            pltpu.VMEM((1, grid_side), jnp.int32),
            pltpu.VMEM((grid_side, 2 * z_span), BF16),
            pltpu.VMEM((owners, share, width), BF16),
            pltpu.SemaphoreType.DMA((4,)),
        ],
        compiler_params=params,
        name="sticks",
    )(
        me,
        *stay(
            coefficients, stick_map, plane_order.reshape(1, grid_side), z_constants(grid_side, z_span)
        ),
    )

    received = exchange(sent, owners, False)

    group = next(g for g in (8, 4, 2, 1) if share % g == 0)
    tables = axis_constants(grid_side, lane_pad)
    total = owners * slots
    columns = pl.pallas_call(
        functools.partial(
            plane_kernel, sources=owners, bands=bands, slots=slots, share=share, group=group
        ),
        in_specs=[in_vmem] * owners + [in_hbm] * 5,
        out_shape=[jax.ShapeDtypeStruct((share, width), BF16)] * owners,
        scratch_shapes=[pltpu.VMEM(potential.shape, F32)]
        + [pltpu.VMEM(t.shape, BF16) for t in tables]
        + [
            pltpu.VMEM((owners, share, width), F32),
            pltpu.VMEM((grid_side // 4, total), F32),
            pltpu.VMEM((total, 2 * lane_pad), BF16),
            pltpu.VMEM((2 * lane_pad, total), BF16),
            pltpu.VMEM((owners, share, width), F32),
            pltpu.SemaphoreType.DMA((4,)),
            pltpu.SemaphoreType.DMA((share // group,)),
        ],
        compiler_params=params,
        name="planes",
    )(*received, *stay(potential, *tables))

    returned = exchange(columns, owners, True)
    return pl.pallas_call(
        functools.partial(column_kernel, owners=owners, slots=slots),
        in_specs=[in_smem] + [in_vmem] * (owners + 2),
        out_shape=jax.ShapeDtypeStruct(coefficients.shape, F32),
        scratch_shapes=[pltpu.VMEM((owners, share, width), BF16)],
        compiler_params=params,
        name="columns",
    )(me, half_len, table, *returned)


def solution(mesh):
    placed = (
        P(("groups", "band", "sub"), None, None, "fft"),
        P(("groups", "fft"), None, None),
        P(None, ("groups", "fft")),
        P("groups"),
    )
    return jax.shard_map(
        body,
        mesh=mesh,
        in_specs=placed,
        out_specs=P(("groups", "band", "sub"), None, None, "fft"),
        check_vma=False,
    )
```

```python
import functools
import math

import jax
import jax.numpy as jnp
import numpy as np
from jax import lax
from jax.experimental import pallas as pl
from jax.experimental.pallas import tpu as pltpu
from jax.sharding import PartitionSpec as P

F32 = jnp.float32
BF16 = jnp.bfloat16
PARAMS = pltpu.CompilerParams(vmem_limit_bytes=28 << 20)
IN_SMEM = pl.BlockSpec(memory_space=pltpu.SMEM)
IN_HBM = pl.BlockSpec(memory_space=pltpu.HBM)
IN_VMEM = pl.BlockSpec(memory_space=pltpu.VMEM)
GROUPS = (8, 4, 2, 1)


def stay(*arrays):
    return tuple(pltpu.with_memory_space_constraint(one, pltpu.HBM) for one in arrays)


def angle_tables(left_ids, right_ids, modulus):
    turns = (left_ids[:, None] * right_ids[None, :]) % modulus
    angles = turns * (2.0 * math.pi / modulus)
    return np.cos(angles), np.sin(angles)


def pad_to(array, rows, cols):
    return np.pad(array, ((0, rows - array.shape[0]), (0, cols - array.shape[1])))


def z_constants(grid_side, z_span):
    freq = (np.arange(z_span) - z_span // 2) % grid_side
    return jnp.asarray(np.concatenate(angle_tables(np.arange(grid_side), freq, grid_side), 1), BF16)


def axis_constants(grid_side, lane_pad):
    half = grid_side // 2
    quarter = half // 2
    grid_ids = np.arange(grid_side)
    compact = np.arange(half)
    window = np.where(compact < quarter, compact, compact + half)
    cos_w, sin_w = angle_tables(window, grid_ids, grid_side)

    def by_high(top, bottom):
        parts = []
        for high in range(2):
            rows = slice(high * quarter, (high + 1) * quarter)
            parts += [top[rows], bottom[rows]]
        return np.concatenate(parts, 0)

    forward_x = np.concatenate([by_high(cos_w, -sin_w).T, by_high(sin_w, cos_w).T], 0)
    pad = functools.partial(pad_to, rows=lane_pad, cols=grid_side)
    forward_y = np.stack(
        [
            np.concatenate([pad(cos_w), pad(-sin_w)], 0),
            np.concatenate([pad(sin_w), pad(cos_w)], 0),
        ]
    )
    inverse_y = np.stack(
        [
            np.concatenate([pad(cos_w).T, pad(-sin_w).T], 1),
            np.concatenate([pad(sin_w).T, pad(cos_w).T], 1),
        ]
    )
    inverse_x = np.stack([by_high(cos_w, -sin_w), by_high(sin_w, cos_w)])
    return tuple(jnp.asarray(t, BF16) for t in (forward_x, forward_y, inverse_y, inverse_x))


def mm(left, right):
    return jnp.dot(left, right, preferred_element_type=F32)


def mm_t(left, right):
    return lax.dot_general(left, right, (((0,), (0,)), ((), ())), preferred_element_type=F32)


def hops(owners):
    return (0,) + tuple(range(owners - 1, 0, -1))


def partner(index, hop, owners):
    return index ^ hop if owners & (owners - 1) == 0 else (index + hop) % owners


def copies_in(sources, targets, sems):
    started = [
        pltpu.make_async_copy(src, dst, sems.at[i]) for i, (src, dst) in enumerate(zip(sources, targets))
    ]
    for one in started:
        one.start()
    return started


def stick_kernel(me, coeff_h, smap_h, order_h, turn_h, *refs, owners, share):
    outs = refs[:owners]
    table, half_len, coeff, smap, order, turn, sticks, sems = refs[owners:]
    started = copies_in((order_h, turn_h, smap_h, coeff_h), (order, turn, smap, coeff), sems)
    bands, _, z_span, slots = coeff.shape
    grid_side = order.shape[1]
    started[0].wait()
    chosen = lax.broadcasted_iota(jnp.int32, (grid_side, grid_side), 0) == order[...]
    chosen = jnp.where(chosen, 1.0, 0.0).astype(BF16)
    started[1].wait()
    rows = mm_t(chosen, turn[...])
    table[...] = rows.T.astype(BF16)
    rows = rows.astype(BF16)
    cos_rows, sin_rows = rows[:, :z_span], rows[:, z_span:]
    lefts = (
        jnp.concatenate([cos_rows, -sin_rows], 1),
        jnp.concatenate([sin_rows, cos_rows], 1),
    )
    started[2].wait()
    entries = lax.broadcasted_iota(jnp.int32, (z_span, slots), 0)
    half = (smap[2:3, :] + 1) // 2 - 1
    half_len[...] = jnp.broadcast_to(half, half_len.shape)
    keep = jnp.abs(entries - z_span // 2) <= half
    started[3].wait()
    for band in range(bands):
        parts = []
        for comp in range(2):
            values = coeff[band, comp].astype(F32)
            parts.append(jnp.where(keep, values, 0.0).astype(BF16))
        masked = jnp.concatenate(parts, 0)
        for comp in range(2):
            found = mm(lefts[comp], masked).astype(BF16)
            col = (band * 2 + comp) * slots
            for owner in range(owners):
                sticks[owner, :, col : col + slots] = found[owner * share : (owner + 1) * share]
    spare = outs[0].shape[0] - share
    x_id = jnp.where(half >= 0, smap[0:1, :], grid_side)
    places = jnp.concatenate([x_id, smap[1:2, :]], 1).astype(F32)
    places = jnp.broadcast_to(places, (spare, 2 * slots)).astype(BF16)
    for out, hop in zip(outs, hops(owners)):
        out[0:share, :] = sticks[partner(me[0], hop, owners)]
        out[share:, 0 : 2 * slots] = places
        if bands > 1:
            out[share:, 2 * slots :] = jnp.zeros((spare, (bands - 1) * 2 * slots), BF16)


def plane_kernel(*refs, sources, bands, slots, share, group):
    recv = refs[:sources]
    pot, fwd_x, fwd_y, inv_y, inv_x = refs[sources : sources + 5]
    outs = refs[sources + 5 : 2 * sources + 5]
    vals, select, low, high_t, high, acc = refs[2 * sources + 5 :]
    grid_side = pot.shape[1]
    half = grid_side // 2
    quarter = half // 2
    lane_pad = high.shape[0] // 2

    live_count = low.shape[1]
    upper = lax.broadcasted_iota(jnp.int32, (slots, slots), 0)
    upper = upper < lax.broadcasted_iota(jnp.int32, (slots, slots), 1)
    upper = jnp.where(upper, 1.0, 0.0).astype(BF16)
    before = jnp.zeros((1, 1), F32)
    gathered = None
    for src in range(sources):
        cols = slice(src * slots, (src + 1) * slots)
        places = recv[src][share:, 0:slots].astype(F32)
        live = jnp.where(places < grid_side, 1.0, 0.0)
        rank = mm(live.astype(BF16), upper)[0:1] + before
        live = live[0:1]
        before = before + jnp.sum(live, axis=1, keepdims=True)
        rank = jnp.where(live > 0.0, rank, -1.0).astype(jnp.int32)
        numbers = lax.broadcasted_iota(jnp.int32, (live_count, slots), 0)
        chosen = jnp.where(numbers == rank, 1.0, 0.0).astype(BF16)
        select[:, cols] = chosen
        pieces = [recv[src][:, i * slots : (i + 1) * slots] for i in range(2 * bands)]
        part = lax.dot_general(
            jnp.concatenate(pieces, 0), chosen, (((1,), (1,)), ((), ())), preferred_element_type=F32
        )
        gathered = part if gathered is None else gathered + part
    vals[...] = gathered
    rows_sent = recv[0].shape[0]

    def compacted(row):
        ids = row.astype(jnp.int32)
        return jnp.clip(jnp.where(ids < quarter, ids, ids - half), 0, half - 1)

    x_id = compacted(gathered[share : share + 1])
    y_id = compacted(gathered[rows_sent + share : rows_sent + share + 1])
    x_high = jnp.where(x_id >= quarter, 1, 0)
    x_low = x_id - x_high * quarter
    rows = lax.broadcasted_iota(jnp.int32, (quarter, live_count), 0)
    low[...] = jnp.where(rows == x_low, 1.0, 0.0)
    rows = lax.broadcasted_iota(jnp.int32, (2 * lane_pad, live_count), 0)
    hot = jnp.where(rows == x_high * lane_pad + y_id, 1.0, 0.0)
    high[...] = hot.astype(BF16)
    high_t[...] = hot.T.astype(BF16)

    def one_group(step):
        base = step * group
        units = [(plane, band) for plane in range(group) for band in range(bands)]
        pairs = [units[i : i + 2] for i in range(0, len(units), 2)]
        low_hot = low[...].astype(BF16)

        def spread(pair):
            stacked = []
            for plane, band in pair:
                for comp in range(2):
                    row = vals[pl.ds((band * 2 + comp) * rows_sent + base + plane, 1), :]
                    stacked.append(jnp.broadcast_to(row, low_hot.shape).astype(BF16) * low_hot)
            spots = mm(jnp.concatenate(stacked, 0), high_t[...]).astype(BF16)
            lanes = []
            for i in range(len(pair)):
                rows = spots[i * half : (i + 1) * half]
                lanes.append(jnp.concatenate([rows[:, :lane_pad], rows[:, lane_pad:]], 0))
            return jnp.concatenate(lanes, 1)

        def along_x(grid):
            return mm(fwd_x[...], grid).astype(BF16)

        def along_y(grid):
            stacked = []
            for i in range(grid.shape[1] // lane_pad):
                cols = slice(i * lane_pad, (i + 1) * lane_pad)
                stacked.append(jnp.concatenate([grid[:grid_side, cols], grid[grid_side:, cols]], 1))
            stacked = jnp.concatenate(stacked, 0)
            return mm(stacked, fwd_y[0]), mm(stacked, fwd_y[1])

        def times_potential(pair, fields):
            real, imag = [], []
            for i, (plane, _) in enumerate(pair):
                rows = slice(i * grid_side, (i + 1) * grid_side)
                field = pot[base + plane]
                real.append((fields[0][rows] * field).astype(BF16))
                imag.append((fields[1][rows] * field).astype(BF16))
            return jnp.concatenate(real, 0), jnp.concatenate(imag, 0)

        def back_y(product):
            return (mm(product[0], inv_y[0]) + mm(product[1], inv_y[1])).astype(BF16)

        def back_x(grid):
            count = grid.shape[0] // grid_side
            total = None
            for comp in range(2):
                cols = slice(comp * lane_pad, (comp + 1) * lane_pad)
                rhs = [grid[i * grid_side : (i + 1) * grid_side, cols] for i in range(count)]
                part = mm(inv_x[comp], jnp.concatenate(rhs, 1))
                total = part if total is None else total + part
            return total.astype(BF16)

        def pick(pair, grid):
            stacked = []
            for i in range(len(pair)):
                cols = slice(i * lane_pad, (i + 1) * lane_pad)
                stacked.append(jnp.concatenate([grid[:half, cols], grid[half:, cols]], 1))
            found = mm(jnp.concatenate(stacked, 0), high[...])
            for i, (plane, band) in enumerate(pair):
                for comp in range(2):
                    start = i * half + comp * quarter
                    line = jnp.sum(found[start : start + quarter] * low[...], axis=0, keepdims=True)
                    acc[pl.ds((band * 2 + comp) * share + base + plane, 1), :] = line

        grids = [spread(pair) for pair in pairs]
        grids = [along_x(grid) for grid in grids]
        fields = [along_y(grid) for grid in grids]
        products = [times_potential(pair, field) for pair, field in zip(pairs, fields)]
        grids = [back_y(product) for product in products]
        grids = [back_x(grid) for grid in grids]
        for pair, grid in zip(pairs, grids):
            pick(pair, grid)

    @pl.loop(0, share // group)
    def _(step):
        one_group(step)

    spread_out = mm(acc[...].astype(BF16), select[...]).astype(BF16)
    for src in range(sources):
        for i in range(2 * bands):
            outs[src][:, i * slots : (i + 1) * slots] = spread_out[
                i * share : (i + 1) * share, src * slots : (src + 1) * slots
            ]


def column_kernel(me, half_len, table, *refs, owners, slots):
    returned, (out, grid) = refs[:owners], refs[owners:]
    bands, _, z_span, _ = out.shape
    for part, hop in zip(returned, hops(owners)):
        grid[partner(me[0], hop, owners)] = part[...]
    entries = lax.broadcasted_iota(jnp.int32, (z_span, slots), 0)
    keep = jnp.abs(entries - z_span // 2) <= half_len[0:1, :]
    grid_side = table.shape[1]
    scale = jnp.where(keep, 1.0 / grid_side**3, 0.0)
    for band in range(bands):
        lines = []
        for comp in range(2):
            col = (band * 2 + comp) * slots
            lines.append(
                jnp.concatenate([grid[owner, :, col : col + slots] for owner in range(owners)], 0)
            )
        by_real = mm(table[...], lines[0])
        by_imag = mm(table[...], lines[1])
        out[band, 0] = (by_real[:z_span] + by_imag[z_span:]) * scale
        out[band, 1] = (by_imag[:z_span] - by_real[z_span:]) * scale


def exchange(parts, owners, back):
    result = [parts[0]]
    for part, hop in zip(parts[1:], hops(owners)[1:]):
        pairs = [(i, partner(i, hop, owners)) for i in range(owners)]
        if back:
            pairs = [(there, here) for here, there in pairs]
        with jax.named_scope(("back" if back else "send") + str(hop)):
            result.append(lax.ppermute(part, "fft", pairs))
    return result


def preload_kernel(*refs):
    count = len(refs) // 2
    for one in copies_in(refs[:count], refs[count : 2 * count], refs[2 * count]):
        one.wait()


def preload(arrays):
    return pl.pallas_call(
        preload_kernel,
        in_specs=[IN_HBM] * len(arrays),
        out_specs=[IN_VMEM] * len(arrays),
        out_shape=[pltpu.VMEM(one.shape, one.dtype) for one in arrays],
        scratch_shapes=[pltpu.SemaphoreType.DMA((len(arrays),))],
        compiler_params=PARAMS,
        name="preload",
    )(*stay(*arrays))


def padded(size):
    return -(-size // 128) * 128


def plane_call(received, potential, tables, bands, slots):
    owners = len(received)
    share, grid_side, _ = potential.shape
    width = bands * 2 * slots
    lane_pad = padded(grid_side // 2)
    group = next(g for g in GROUPS if share % g == 0)
    total = owners * slots
    live = total // 2
    return pl.pallas_call(
        functools.partial(
            plane_kernel, sources=owners, bands=bands, slots=slots, share=share, group=group
        ),
        in_specs=[IN_VMEM] * (owners + 5),
        out_shape=[jax.ShapeDtypeStruct((share, width), BF16)] * owners,
        scratch_shapes=[
            pltpu.VMEM((2 * bands * received[0].shape[0], live), F32),
            pltpu.VMEM((live, total), BF16),
            pltpu.VMEM((grid_side // 4, live), F32),
            pltpu.VMEM((live, 2 * lane_pad), BF16),
            pltpu.VMEM((2 * lane_pad, live), BF16),
            pltpu.VMEM((2 * bands * share, live), F32),
        ],
        compiler_params=PARAMS,
        name="planes",
    )(*received, potential, *tables)


def body(coefficients, potential, stick_map, plane_order):
    bands, _, z_span, slots = coefficients.shape
    share, grid_side, _ = potential.shape
    owners = lax.axis_size("fft")
    width = bands * 2 * slots
    rows_sent = (share // 8 + 1) * 8
    me = lax.axis_index("fft").astype(jnp.int32).reshape(1)

    *sent, table, half_len = pl.pallas_call(
        functools.partial(stick_kernel, owners=owners, share=share),
        in_specs=[IN_SMEM] + [IN_HBM] * 4,
        out_shape=[jax.ShapeDtypeStruct((rows_sent, width), BF16)] * owners
        + [
            jax.ShapeDtypeStruct((2 * z_span, grid_side), BF16),
            jax.ShapeDtypeStruct((8, slots), jnp.int32),
        ],
        scratch_shapes=[
            pltpu.VMEM(coefficients.shape, BF16),
            pltpu.VMEM(stick_map.shape, jnp.int32),
            pltpu.VMEM((1, grid_side), jnp.int32),
            pltpu.VMEM((grid_side, 2 * z_span), BF16),
            pltpu.VMEM((owners, share, width), BF16),
            pltpu.SemaphoreType.DMA((4,)),
        ],
        compiler_params=PARAMS,
        name="sticks",
    )(
        me,
        *stay(
            coefficients, stick_map, plane_order.reshape(1, grid_side), z_constants(grid_side, z_span)
        ),
    )

    loaded = preload([potential, *axis_constants(grid_side, padded(grid_side // 2))])
    received = exchange(sent, owners, False)

    columns = plane_call(received, loaded[0], loaded[1:], bands, slots)
    returned = exchange(columns, owners, True)
    return pl.pallas_call(
        functools.partial(column_kernel, owners=owners, slots=slots),
        in_specs=[IN_SMEM] + [IN_VMEM] * (owners + 2),
        out_shape=jax.ShapeDtypeStruct(coefficients.shape, F32),
        scratch_shapes=[pltpu.VMEM((owners, share, width), BF16)],
        compiler_params=PARAMS,
        name="columns",
    )(me, half_len, table, *returned)


def solution(mesh):
    placed = (
        P(("groups", "band", "sub"), None, None, "fft"),
        P(("groups", "fft"), None, None),
        P(None, ("groups", "fft")),
        P("groups"),
    )
    return jax.shard_map(
        body,
        mesh=mesh,
        in_specs=placed,
        out_specs=P(("groups", "band", "sub"), None, None, "fft"),
        check_vma=False,
    )
```

```python
import functools
import math

import jax
import jax.numpy as jnp
import numpy as np
from jax import lax
from jax.experimental import pallas as pl
from jax.experimental.pallas import tpu as pltpu
from jax.sharding import PartitionSpec as P

F32 = jnp.float32
BF16 = jnp.bfloat16
PARAMS = pltpu.CompilerParams(vmem_limit_bytes=28 << 20)
IN_SMEM = pl.BlockSpec(memory_space=pltpu.SMEM)
IN_HBM = pl.BlockSpec(memory_space=pltpu.HBM)
IN_VMEM = pl.BlockSpec(memory_space=pltpu.VMEM)
GROUPS = (48, 24, 16, 12, 8, 4, 2, 1)


def stay(*arrays):
    return tuple(pltpu.with_memory_space_constraint(one, pltpu.HBM) for one in arrays)


def angle_tables(left_ids, right_ids, modulus):
    turns = (left_ids[:, None] * right_ids[None, :]) % modulus
    angles = turns * (2.0 * math.pi / modulus)
    return np.cos(angles), np.sin(angles)


def pad_to(array, rows, cols):
    return np.pad(array, ((0, rows - array.shape[0]), (0, cols - array.shape[1])))


def z_constants(grid_side, z_span):
    freq = (np.arange(z_span) - z_span // 2) % grid_side
    return jnp.asarray(np.concatenate(angle_tables(np.arange(grid_side), freq, grid_side), 1), BF16)


def axis_constants(grid_side, lane_pad):
    half = grid_side // 2
    quarter = half // 2
    grid_ids = np.arange(grid_side)
    compact = np.arange(half)
    window = np.where(compact < quarter, compact, compact + half)
    cos_w, sin_w = angle_tables(window, grid_ids, grid_side)

    def by_high(top, bottom):
        parts = []
        for high in range(2):
            rows = slice(high * quarter, (high + 1) * quarter)
            parts += [top[rows], bottom[rows]]
        return np.concatenate(parts, 0)

    forward_x = np.concatenate([by_high(cos_w, -sin_w).T, by_high(sin_w, cos_w).T], 0)
    pad = functools.partial(pad_to, rows=lane_pad, cols=grid_side)
    forward_y = np.stack(
        [
            np.concatenate([pad(cos_w), pad(-sin_w)], 0),
            np.concatenate([pad(sin_w), pad(cos_w)], 0),
        ]
    )
    inverse_y = np.stack(
        [
            np.concatenate([pad(cos_w).T, pad(-sin_w).T], 1),
            np.concatenate([pad(sin_w).T, pad(cos_w).T], 1),
        ]
    )
    inverse_x = np.stack([by_high(cos_w, -sin_w), by_high(sin_w, cos_w)])
    return tuple(jnp.asarray(t, BF16) for t in (forward_x, forward_y, inverse_y, inverse_x))


def mm(left, right):
    return jnp.dot(left, right, preferred_element_type=F32)


def mm_t(left, right):
    return lax.dot_general(left, right, (((0,), (0,)), ((), ())), preferred_element_type=F32)


def one_hot_columns(ids, count):
    rows = lax.broadcasted_iota(jnp.int32, (count, ids.shape[1]), 0).astype(jnp.int16)
    ids = jnp.broadcast_to(ids, (16, ids.shape[1])).astype(jnp.int16)
    ids = jnp.concatenate([ids] * (count // 16), 0)
    return jnp.where(rows == ids, jnp.ones((), BF16), jnp.zeros((), BF16))


def hops(owners):
    return (0,) + tuple(range(owners - 1, 0, -1))


def partner(index, hop, owners):
    return index ^ hop if owners & (owners - 1) == 0 else (index + hop) % owners


def copies_in(sources, targets, sems):
    started = [
        pltpu.make_async_copy(src, dst, sems.at[i]) for i, (src, dst) in enumerate(zip(sources, targets))
    ]
    for one in started:
        one.start()
    return started


def stick_kernel(me, coeff_h, smap_h, order_h, turn_h, *refs, owners, share):
    outs = refs[:owners]
    coeff, smap, order, turn, sticks, sems = refs[owners:]
    started = copies_in((order_h, turn_h, smap_h, coeff_h), (order, turn, smap, coeff), sems)
    bands, _, z_span, slots = coeff.shape
    grid_side = order.shape[1]
    started[0].wait()
    chosen = one_hot_columns(order[...], grid_side)
    started[1].wait()
    rows = mm_t(chosen, turn[...]).astype(BF16)
    cos_rows, sin_rows = rows[:, :z_span], rows[:, z_span:]
    lefts = (
        jnp.concatenate([cos_rows, -sin_rows], 1),
        jnp.concatenate([sin_rows, cos_rows], 1),
    )
    started[2].wait()
    entries = lax.broadcasted_iota(jnp.int32, (z_span, slots), 0)
    half = (smap[2:3, :] + 1) // 2 - 1
    keep = jnp.abs(entries - z_span // 2) <= half
    started[3].wait()
    for band in range(bands):
        parts = []
        for comp in range(2):
            values = coeff[band, comp].astype(F32)
            parts.append(jnp.where(keep, values, 0.0).astype(BF16))
        masked = jnp.concatenate(parts, 0)
        for comp in range(2):
            found = mm(lefts[comp], masked).astype(BF16)
            col = (band * 2 + comp) * slots
            for owner in range(owners):
                sticks[owner, :, col : col + slots] = found[owner * share : (owner + 1) * share]
    spare = outs[0].shape[0] - share
    live = jnp.where(half >= 0, 1.0, 0.0)
    upper = lax.broadcasted_iota(jnp.int32, (slots, slots), 0)
    upper = upper < lax.broadcasted_iota(jnp.int32, (slots, slots), 1)
    upper = jnp.where(upper, 1.0, 0.0).astype(BF16)
    number = mm(jnp.broadcast_to(live, (8, slots)).astype(BF16), upper)[0:1]
    number = jnp.where(half >= 0, number, -1.0)
    count = jnp.broadcast_to(jnp.sum(live, axis=1, keepdims=True), (1, slots))
    places = jnp.concatenate(
        [
            jnp.concatenate([smap[0:1, :], smap[1:2, :]], 1).astype(F32),
            jnp.concatenate([number, count], 1),
            jnp.zeros((spare - 2, 2 * slots), F32),
        ],
        0,
    ).astype(BF16)
    for out, hop in zip(outs, hops(owners)):
        out[0:share, :] = sticks[partner(me[0], hop, owners)]
        out[share:, 0 : 2 * slots] = places
        if bands > 1:
            out[share:, 2 * slots :] = jnp.zeros((spare, (bands - 1) * 2 * slots), BF16)


def plane_kernel(*refs, sources, bands, slots, share, group):
    recv = refs[:sources]
    pot, fwd_x, fwd_y, inv_y, inv_x = refs[sources : sources + 5]
    outs = refs[sources + 5 : 2 * sources + 5]
    vals, select, low, high_t, high, acc = refs[2 * sources + 5 :]
    grid_side = pot.shape[1]
    half = grid_side // 2
    quarter = half // 2
    lane_pad = high.shape[0] // 2

    live_count = low.shape[1]
    before = jnp.zeros((1, slots), F32)
    gathered = None
    for src in range(sources):
        cols = slice(src * slots, (src + 1) * slots)
        places = recv[src][share:, :].astype(F32)
        number = places[1:2, 0:slots]
        number = jnp.where(number >= 0.0, number + before, -1.0)
        before = before + places[1:2, slots : 2 * slots]
        chosen = one_hot_columns(number.astype(jnp.int32), live_count)
        select[:, cols] = chosen
        pieces = [recv[src][:, i * slots : (i + 1) * slots] for i in range(2 * bands)]
        part = lax.dot_general(
            jnp.concatenate(pieces, 0), chosen, (((1,), (1,)), ((), ())), preferred_element_type=F32
        )
        gathered = part if gathered is None else gathered + part
    vals[...] = gathered
    rows_sent = recv[0].shape[0]

    def compacted(row):
        ids = row.astype(jnp.int32)
        return jnp.clip(jnp.where(ids < quarter, ids, ids - half), 0, half - 1)

    x_id = compacted(gathered[share : share + 1])
    y_id = compacted(gathered[rows_sent + share : rows_sent + share + 1])
    x_high = jnp.where(x_id >= quarter, 1, 0)
    x_low = x_id - x_high * quarter
    rows = lax.broadcasted_iota(jnp.int32, (quarter, live_count), 0)
    low[...] = jnp.where(rows == x_low, 1.0, 0.0)
    hot = one_hot_columns(x_high * lane_pad + y_id, 2 * lane_pad)
    high[...] = hot
    high_t[...] = hot.T

    def one_group(step):
        base = step * group
        units = [(plane, band) for plane in range(group) for band in range(bands)]
        pairs = [units[i : i + 2] for i in range(0, len(units), 2)]
        low_hot = low[...].astype(BF16)

        def spread(pair):
            stacked = []
            for plane, band in pair:
                for comp in range(2):
                    row = vals[pl.ds((band * 2 + comp) * rows_sent + base + plane, 1), :]
                    stacked.append(jnp.broadcast_to(row, low_hot.shape).astype(BF16) * low_hot)
            spots = mm(jnp.concatenate(stacked, 0), high_t[...]).astype(BF16)
            lanes = []
            for i in range(len(pair)):
                rows = spots[i * half : (i + 1) * half]
                lanes.append(jnp.concatenate([rows[:, :lane_pad], rows[:, lane_pad:]], 0))
            return jnp.concatenate(lanes, 1)

        def along_x(grid):
            return mm(fwd_x[...], grid).astype(BF16)

        def along_y(grid):
            stacked = []
            for i in range(grid.shape[1] // lane_pad):
                cols = slice(i * lane_pad, (i + 1) * lane_pad)
                stacked.append(jnp.concatenate([grid[:grid_side, cols], grid[grid_side:, cols]], 1))
            stacked = jnp.concatenate(stacked, 0)
            return mm(stacked, fwd_y[0]), mm(stacked, fwd_y[1])

        def times_potential(pair, fields):
            real, imag = [], []
            for i, (plane, _) in enumerate(pair):
                rows = slice(i * grid_side, (i + 1) * grid_side)
                field = pot[base + plane]
                real.append((fields[0][rows] * field).astype(BF16))
                imag.append((fields[1][rows] * field).astype(BF16))
            return jnp.concatenate(real, 0), jnp.concatenate(imag, 0)

        def back_y(product):
            return (mm(product[0], inv_y[0]) + mm(product[1], inv_y[1])).astype(BF16)

        def back_x(grid):
            count = grid.shape[0] // grid_side
            total = None
            for comp in range(2):
                cols = slice(comp * lane_pad, (comp + 1) * lane_pad)
                rhs = [grid[i * grid_side : (i + 1) * grid_side, cols] for i in range(count)]
                part = mm(inv_x[comp], jnp.concatenate(rhs, 1))
                total = part if total is None else total + part
            return total.astype(BF16)

        def pick(pair, grid):
            stacked = []
            for i in range(len(pair)):
                cols = slice(i * lane_pad, (i + 1) * lane_pad)
                stacked.append(jnp.concatenate([grid[:half, cols], grid[half:, cols]], 1))
            found = mm(jnp.concatenate(stacked, 0), high[...])
            for i, (plane, band) in enumerate(pair):
                for comp in range(2):
                    start = i * half + comp * quarter
                    line = jnp.sum(found[start : start + quarter] * low[...], axis=0, keepdims=True)
                    acc[pl.ds((band * 2 + comp) * share + base + plane, 1), :] = line

        grids = [spread(pair) for pair in pairs]
        grids = [along_x(grid) for grid in grids]
        fields = [along_y(grid) for grid in grids]
        products = [times_potential(pair, field) for pair, field in zip(pairs, fields)]
        grids = [back_y(product) for product in products]
        grids = [back_x(grid) for grid in grids]
        for pair, grid in zip(pairs, grids):
            pick(pair, grid)

    if group == share:
        one_group(0)
    else:
        pl.loop(0, share // group)(one_group)

    spread_out = mm(acc[...].astype(BF16), select[...]).astype(BF16)
    for src in range(sources):
        for i in range(2 * bands):
            outs[src][:, i * slots : (i + 1) * slots] = spread_out[
                i * share : (i + 1) * share, src * slots : (src + 1) * slots
            ]


def column_kernel(me, half_len, table, *refs, owners, slots):
    returned, (out, grid) = refs[:owners], refs[owners:]
    bands, _, z_span, _ = out.shape
    for part, hop in zip(returned, hops(owners)):
        grid[partner(me[0], hop, owners)] = part[...]
    entries = lax.broadcasted_iota(jnp.int32, (z_span, slots), 0)
    keep = jnp.abs(entries - z_span // 2) <= half_len[0:1, :]
    grid_side = table.shape[1]
    scale = jnp.where(keep, 1.0 / grid_side**3, 0.0)
    for band in range(bands):
        lines = []
        for comp in range(2):
            col = (band * 2 + comp) * slots
            lines.append(
                jnp.concatenate([grid[owner, :, col : col + slots] for owner in range(owners)], 0)
            )
        by_real = mm(table[...], lines[0])
        by_imag = mm(table[...], lines[1])
        out[band, 0] = (by_real[:z_span] + by_imag[z_span:]) * scale
        out[band, 1] = (by_imag[:z_span] - by_real[z_span:]) * scale


def exchange(parts, owners, back):
    result = [parts[0]]
    for part, hop in zip(parts[1:], hops(owners)[1:]):
        pairs = [(i, partner(i, hop, owners)) for i in range(owners)]
        if back:
            pairs = [(there, here) for here, there in pairs]
        with jax.named_scope(("back" if back else "send") + str(hop)):
            result.append(lax.ppermute(part, "fft", pairs))
    return result


def preload_kernel(order_h, turn_h, smap_h, *refs):
    count = (len(refs) - 6) // 2
    table, half_len, order, turn, smap, sems = refs[2 * count :]
    started = copies_in(
        (order_h, turn_h, smap_h, *refs[:count]), (order, turn, smap, *refs[count : 2 * count]), sems
    )
    for one in started[:3]:
        one.wait()
    chosen = one_hot_columns(order[...], order.shape[1])
    table[...] = mm_t(turn[...], chosen).astype(BF16)
    half = (smap[2:3, :] + 1) // 2 - 1
    half_len[...] = jnp.broadcast_to(half, half_len.shape)
    for one in started[3:]:
        one.wait()


def preload(order, turn, smap, arrays):
    out = [(one.shape, one.dtype) for one in arrays]
    out += [((turn.shape[1], order.shape[1]), BF16), ((8, smap.shape[1]), jnp.int32)]
    *loaded, table, half_len = pl.pallas_call(
        preload_kernel,
        in_specs=[IN_HBM] * (len(arrays) + 3),
        out_specs=[IN_VMEM] * len(out),
        out_shape=[pltpu.VMEM(*one) for one in out],
        scratch_shapes=[pltpu.VMEM(one.shape, one.dtype) for one in (order, turn, smap)]
        + [pltpu.SemaphoreType.DMA((len(arrays) + 3,))],
        compiler_params=PARAMS,
        name="preload",
    )(*stay(order, turn, smap, *arrays))
    return loaded, table, half_len


def padded(size):
    return -(-size // 128) * 128


def plane_call(received, potential, tables, bands, slots):
    owners = len(received)
    share, grid_side, _ = potential.shape
    width = bands * 2 * slots
    lane_pad = padded(grid_side // 2)
    group = next(g for g in GROUPS if share % g == 0)
    total = owners * slots
    live = total // 2
    return pl.pallas_call(
        functools.partial(
            plane_kernel, sources=owners, bands=bands, slots=slots, share=share, group=group
        ),
        in_specs=[IN_VMEM] * (owners + 5),
        out_shape=[jax.ShapeDtypeStruct((share, width), BF16)] * owners,
        scratch_shapes=[
            pltpu.VMEM((2 * bands * received[0].shape[0], live), F32),
            pltpu.VMEM((live, total), BF16),
            pltpu.VMEM((grid_side // 4, live), F32),
            pltpu.VMEM((live, 2 * lane_pad), BF16),
            pltpu.VMEM((2 * lane_pad, live), BF16),
            pltpu.VMEM((2 * bands * share, live), F32),
        ],
        compiler_params=PARAMS,
        name="planes",
    )(*received, potential, *tables)


def body(coefficients, potential, stick_map, plane_order):
    bands, _, z_span, slots = coefficients.shape
    share, grid_side, _ = potential.shape
    owners = lax.axis_size("fft")
    width = bands * 2 * slots
    rows_sent = -(-(share + 2) // 8) * 8
    me = lax.axis_index("fft").astype(jnp.int32).reshape(1)

    order = plane_order.reshape(1, grid_side)
    turn = z_constants(grid_side, z_span)

    sent = pl.pallas_call(
        functools.partial(stick_kernel, owners=owners, share=share),
        in_specs=[IN_SMEM] + [IN_HBM] * 4,
        out_shape=[jax.ShapeDtypeStruct((rows_sent, width), BF16)] * owners,
        scratch_shapes=[
            pltpu.VMEM(coefficients.shape, BF16),
            pltpu.VMEM(stick_map.shape, jnp.int32),
            pltpu.VMEM(order.shape, jnp.int32),
            pltpu.VMEM(turn.shape, BF16),
            pltpu.VMEM((owners, share, width), BF16),
            pltpu.SemaphoreType.DMA((4,)),
        ],
        compiler_params=PARAMS,
        name="sticks",
    )(me, *stay(coefficients, stick_map, order, turn))

    axis_tables = axis_constants(grid_side, padded(grid_side // 2))
    loaded, table, half_len = preload(order, turn, stick_map, [potential, *axis_tables])
    received = exchange(sent, owners, False)

    columns = plane_call(received, loaded[0], loaded[1:], bands, slots)
    returned = exchange(columns, owners, True)
    return pl.pallas_call(
        functools.partial(column_kernel, owners=owners, slots=slots),
        in_specs=[IN_SMEM] + [IN_VMEM] * (owners + 2),
        out_shape=jax.ShapeDtypeStruct(coefficients.shape, F32),
        scratch_shapes=[pltpu.VMEM((owners, share, width), BF16)],
        compiler_params=PARAMS,
        name="columns",
    )(me, half_len, table, *returned)


def solution(mesh):
    placed = (
        P(("groups", "band", "sub"), None, None, "fft"),
        P(("groups", "fft"), None, None),
        P(None, ("groups", "fft")),
        P("groups"),
    )
    return jax.shard_map(
        body,
        mesh=mesh,
        in_specs=placed,
        out_specs=P(("groups", "band", "sub"), None, None, "fft"),
        check_vma=False,
    )
```

```python
import functools
import math

import jax
import jax.numpy as jnp
import numpy as np
from jax import lax
from jax.experimental import pallas as pl
from jax.experimental.pallas import tpu as pltpu
from jax.sharding import PartitionSpec as P

F32 = jnp.float32
BF16 = jnp.bfloat16
PARAMS = pltpu.CompilerParams(vmem_limit_bytes=28 << 20)
IN_SMEM = pl.BlockSpec(memory_space=pltpu.SMEM)
IN_HBM = pl.BlockSpec(memory_space=pltpu.HBM)
IN_VMEM = pl.BlockSpec(memory_space=pltpu.VMEM)
GROUPS = (24, 16, 12, 8, 4, 2)


def stay(*arrays):
    return tuple(pltpu.with_memory_space_constraint(one, pltpu.HBM) for one in arrays)


def angle_tables(left_ids, right_ids, modulus):
    turns = (left_ids[:, None] * right_ids[None, :]) % modulus
    angles = turns * (2.0 * math.pi / modulus)
    return np.cos(angles), np.sin(angles)


def z_constants(grid_side, z_span):
    freq = (np.arange(z_span) - z_span // 2) % grid_side
    return jnp.asarray(np.concatenate(angle_tables(np.arange(grid_side), freq, grid_side), 1), BF16)


def axis_constants(grid_side, lane_pad, pair_pad):
    half = grid_side // 2
    compact = np.arange(half)
    window = np.where(compact < half // 2, compact, compact + half)
    cos_w, sin_w = angle_tables(window, np.arange(grid_side), grid_side)

    def placed(table, phase):
        spare = pair_pad - grid_side
        lanes = (0, spare) if phase == 0 else (spare, 0)
        return np.pad(table, ((0, lane_pad - half), lanes))

    forward_y, inverse_y = [], []
    for phase in range(2):
        cos_p, sin_p = placed(cos_w, phase), placed(sin_w, phase)
        forward_y.append([np.concatenate([cos_p, -sin_p], 0), np.concatenate([sin_p, cos_p], 0)])
        inverse_y.append([np.concatenate([cos_p.T, -sin_p.T], 1), np.concatenate([sin_p.T, cos_p.T], 1)])
    forward_x = np.concatenate(
        [np.concatenate([cos_w.T, -sin_w.T], 1), np.concatenate([sin_w.T, cos_w.T], 1)], 0
    )
    inverse_x = [np.concatenate([cos_w, -sin_w], 0), np.concatenate([sin_w, cos_w], 0)]
    return tuple(jnp.asarray(np.array(t), BF16) for t in (forward_x, forward_y, inverse_y, inverse_x))


def mm(left, right):
    return jnp.dot(left, right, preferred_element_type=F32)


def mm_t(left, right):
    return lax.dot_general(left, right, (((0,), (0,)), ((), ())), preferred_element_type=F32)


def one_hot_columns(ids, count):
    rows = lax.broadcasted_iota(jnp.int32, (count, ids.shape[1]), 0).astype(jnp.int16)
    ids = jnp.broadcast_to(ids, (16, ids.shape[1])).astype(jnp.int16)
    ids = jnp.concatenate([ids] * (count // 16), 0)
    return jnp.where(rows == ids, jnp.ones((), BF16), jnp.zeros((), BF16))


def hops(owners):
    return (0,) + tuple(range(owners - 1, 0, -1))


def partner(index, hop, owners):
    return index ^ hop if owners & (owners - 1) == 0 else (index + hop) % owners


def copies_in(sources, targets, sems):
    started = [
        pltpu.make_async_copy(src, dst, sems.at[i]) for i, (src, dst) in enumerate(zip(sources, targets))
    ]
    for one in started:
        one.start()
    return started


def stick_kernel(me, coeff_h, smap_h, order_h, turn_h, *refs, owners, share):
    outs = refs[:owners]
    coeff, smap, order, turn, sticks, sems = refs[owners:]
    started = copies_in((order_h, turn_h, smap_h, coeff_h), (order, turn, smap, coeff), sems)
    bands, _, z_span, slots = coeff.shape
    grid_side = order.shape[1]
    started[0].wait()
    chosen = one_hot_columns(order[...], grid_side)
    started[1].wait()
    rows = mm_t(chosen, turn[...]).astype(BF16)
    cos_rows, sin_rows = rows[:, :z_span], rows[:, z_span:]
    lefts = (
        jnp.concatenate([cos_rows, -sin_rows], 1),
        jnp.concatenate([sin_rows, cos_rows], 1),
    )
    started[2].wait()
    entries = lax.broadcasted_iota(jnp.int32, (z_span, slots), 0)
    half = (smap[2:3, :] + 1) // 2 - 1
    keep = jnp.abs(entries - z_span // 2) <= half
    started[3].wait()
    for band in range(bands):
        parts = []
        for comp in range(2):
            values = coeff[band, comp].astype(F32)
            parts.append(jnp.where(keep, values, 0.0).astype(BF16))
        masked = jnp.concatenate(parts, 0)
        for comp in range(2):
            found = mm(lefts[comp], masked).astype(BF16)
            col = (band * 2 + comp) * slots
            for owner in range(owners):
                sticks[owner, :, col : col + slots] = found[owner * share : (owner + 1) * share]
    spare = outs[0].shape[0] - share
    live = jnp.where(half >= 0, 1.0, 0.0)
    upper = lax.broadcasted_iota(jnp.int32, (slots, slots), 0)
    upper = upper < lax.broadcasted_iota(jnp.int32, (slots, slots), 1)
    upper = jnp.where(upper, 1.0, 0.0).astype(BF16)
    number = mm(jnp.broadcast_to(live, (8, slots)).astype(BF16), upper)[0:1]
    number = jnp.where(half >= 0, number, -1.0)
    count = jnp.broadcast_to(jnp.sum(live, axis=1, keepdims=True), (1, slots))
    places = jnp.concatenate(
        [
            jnp.concatenate([smap[0:1, :], smap[1:2, :]], 1).astype(F32),
            jnp.concatenate([number, count], 1),
            jnp.zeros((spare - 2, 2 * slots), F32),
        ],
        0,
    ).astype(BF16)
    for out, hop in zip(outs, hops(owners)):
        out[0:share, :] = sticks[partner(me[0], hop, owners)]
        out[share:, 0 : 2 * slots] = places
        if bands > 1:
            out[share:, 2 * slots :] = jnp.zeros((spare, (bands - 1) * 2 * slots), BF16)


def plane_kernel(*refs, sources, bands, slots, share, group):
    recv = refs[:sources]
    pot, fwd_x, fwd_y, inv_y, inv_x = refs[sources : sources + 5]
    outs = refs[sources + 5 : 2 * sources + 5]
    vals, select, low, high_t, high, acc = refs[2 * sources + 5 :]
    grid_side = pot.shape[1]
    half = grid_side // 2
    quarter = half // 2
    lane_pad = high.shape[0] // 2
    pair_pad = fwd_y.shape[3]
    overlap = 2 * grid_side - pair_pad

    live_count = low.shape[1]
    before = jnp.zeros((1, slots), F32)
    gathered = None
    for src in range(sources):
        cols = slice(src * slots, (src + 1) * slots)
        places = recv[src][share:, :].astype(F32)
        number = places[1:2, 0:slots]
        number = jnp.where(number >= 0.0, number + before, -1.0)
        before = before + places[1:2, slots : 2 * slots]
        chosen = one_hot_columns(number.astype(jnp.int32), live_count)
        select[:, cols] = chosen
        pieces = [recv[src][:, i * slots : (i + 1) * slots] for i in range(2 * bands)]
        part = lax.dot_general(
            jnp.concatenate(pieces, 0), chosen, (((1,), (1,)), ((), ())), preferred_element_type=F32
        )
        gathered = part if gathered is None else gathered + part
    vals[...] = gathered
    rows_sent = recv[0].shape[0]

    def compacted(row):
        ids = row.astype(jnp.int32)
        return jnp.clip(jnp.where(ids < quarter, ids, ids - half), 0, half - 1)

    x_id = compacted(gathered[share : share + 1])
    y_id = compacted(gathered[rows_sent + share : rows_sent + share + 1])
    x_high = jnp.where(x_id >= quarter, 1, 0)
    x_low = x_id - x_high * quarter
    rows = lax.broadcasted_iota(jnp.int32, (quarter, live_count), 0)
    low[...] = jnp.where(rows == x_low, 1.0, 0.0)
    hot = one_hot_columns(x_high * lane_pad + y_id, 2 * lane_pad)
    high[...] = hot
    high_t[...] = hot.T

    def one_group(step):
        base = step * group
        pairs = [((p, band), (p + 1, band)) for p in range(0, group, 2) for band in range(bands)]
        bundles = [pairs[i : i + 2] for i in range(0, len(pairs), 2)]
        low_hot = low[...].astype(BF16)

        def by_phase(bundle):
            return [[pair[phase] for pair in bundle] for phase in range(2)]

        def spread(units):
            stacked = []
            for plane, band in units:
                for comp in range(2):
                    row = vals[pl.ds((band * 2 + comp) * rows_sent + base + plane, 1), :]
                    stacked.append(jnp.broadcast_to(row, low_hot.shape).astype(BF16) * low_hot)
            spots = mm(jnp.concatenate(stacked, 0), high_t[...]).astype(BF16)
            rows = []
            for i in range(len(units)):
                real = spots[i * half : i * half + quarter]
                imag = spots[i * half + quarter : (i + 1) * half]
                for lanes in (slice(0, lane_pad), slice(lane_pad, 2 * lane_pad)):
                    rows.append(jnp.concatenate([real[:, lanes], imag[:, lanes]], 1))
            return jnp.concatenate(rows, 0)

        def along_y(grids):
            parts = []
            for comp in range(2):
                found = [mm(grid, fwd_y[phase, comp]).astype(BF16) for phase, grid in enumerate(grids)]
                lanes = []
                for i in range(found[0].shape[0] // half):
                    first, second = (one[i * half : (i + 1) * half] for one in found)
                    lanes += [first[:, :overlap], first[:, overlap:] + second[:, :-overlap]]
                    lanes.append(second[:, -overlap:])
                parts.append(jnp.concatenate(lanes, 1))
            return jnp.concatenate(parts, 0)

        def along_x(bundle, grid):
            fields = mm(fwd_x[...], grid)
            field = jnp.concatenate([pot[base + plane] for pair in bundle for plane, _ in pair], 1)
            return [
                (fields[comp * grid_side : (comp + 1) * grid_side] * field).astype(BF16)
                for comp in range(2)
            ]

        def back_x(product):
            return (mm(inv_x[0], product[0]) + mm(inv_x[1], product[1])).astype(BF16)

        def back_y(grid, count):
            result = []
            for phase in range(2):
                total = None
                for comp in range(2):
                    rows = []
                    for i in range(count):
                        start = i * 2 * grid_side + phase * overlap
                        rows.append(grid[comp * half : (comp + 1) * half, start : start + pair_pad])
                    part = mm(jnp.concatenate(rows, 0), inv_y[phase, comp])
                    total = part if total is None else total + part
                result.append(total.astype(BF16))
            return result

        def pick(units, grid):
            stacked = []
            for i in range(len(units)):
                top = grid[i * half : i * half + quarter]
                bottom = grid[i * half + quarter : (i + 1) * half]
                for lanes in (slice(0, lane_pad), slice(lane_pad, 2 * lane_pad)):
                    stacked.append(jnp.concatenate([top[:, lanes], bottom[:, lanes]], 1))
            found = mm(jnp.concatenate(stacked, 0), high[...])
            for i, (plane, band) in enumerate(units):
                for comp in range(2):
                    start = i * half + comp * quarter
                    line = jnp.sum(found[start : start + quarter] * low[...], axis=0, keepdims=True)
                    acc[pl.ds((band * 2 + comp) * share + base + plane, 1), :] = line

        grids = [[spread(units) for units in by_phase(bundle)] for bundle in bundles]
        grids = [along_y(grid) for grid in grids]
        products = [along_x(bundle, grid) for bundle, grid in zip(bundles, grids)]
        grids = [back_x(product) for product in products]
        grids = [back_y(grid, len(bundle)) for bundle, grid in zip(bundles, grids)]
        for bundle, grid in zip(bundles, grids):
            for units, part in zip(by_phase(bundle), grid):
                pick(units, part)

    if group == share:
        one_group(0)
    else:
        pl.loop(0, share // group)(one_group)

    spread_out = mm(acc[...].astype(BF16), select[...]).astype(BF16)
    for src in range(sources):
        for i in range(2 * bands):
            outs[src][:, i * slots : (i + 1) * slots] = spread_out[
                i * share : (i + 1) * share, src * slots : (src + 1) * slots
            ]


def column_kernel(me, half_len, table, *refs, owners, slots):
    returned, (out, grid) = refs[:owners], refs[owners:]
    bands, _, z_span, _ = out.shape
    for part, hop in zip(returned, hops(owners)):
        grid[partner(me[0], hop, owners)] = part[...]
    entries = lax.broadcasted_iota(jnp.int32, (z_span, slots), 0)
    keep = jnp.abs(entries - z_span // 2) <= half_len[0:1, :]
    grid_side = table.shape[1]
    scale = jnp.where(keep, 1.0 / grid_side**3, 0.0)
    for band in range(bands):
        lines = []
        for comp in range(2):
            col = (band * 2 + comp) * slots
            lines.append(
                jnp.concatenate([grid[owner, :, col : col + slots] for owner in range(owners)], 0)
            )
        by_real = mm(table[...], lines[0])
        by_imag = mm(table[...], lines[1])
        out[band, 0] = (by_real[:z_span] + by_imag[z_span:]) * scale
        out[band, 1] = (by_imag[:z_span] - by_real[z_span:]) * scale


def exchange(parts, owners, back):
    result = [parts[0]]
    for part, hop in zip(parts[1:], hops(owners)[1:]):
        pairs = [(i, partner(i, hop, owners)) for i in range(owners)]
        if back:
            pairs = [(there, here) for here, there in pairs]
        with jax.named_scope(("back" if back else "send") + str(hop)):
            result.append(lax.ppermute(part, "fft", pairs))
    return result


def preload_kernel(order_h, turn_h, smap_h, *refs):
    count = (len(refs) - 6) // 2
    table, half_len, order, turn, smap, sems = refs[2 * count :]
    started = copies_in(
        (order_h, turn_h, smap_h, *refs[:count]), (order, turn, smap, *refs[count : 2 * count]), sems
    )
    for one in started[:3]:
        one.wait()
    chosen = one_hot_columns(order[...], order.shape[1])
    table[...] = mm_t(turn[...], chosen).astype(BF16)
    half = (smap[2:3, :] + 1) // 2 - 1
    half_len[...] = jnp.broadcast_to(half, half_len.shape)
    for one in started[3:]:
        one.wait()


def preload(order, turn, smap, arrays):
    out = [(one.shape, one.dtype) for one in arrays]
    out += [((turn.shape[1], order.shape[1]), BF16), ((8, smap.shape[1]), jnp.int32)]
    *loaded, table, half_len = pl.pallas_call(
        preload_kernel,
        in_specs=[IN_HBM] * (len(arrays) + 3),
        out_specs=[IN_VMEM] * len(out),
        out_shape=[pltpu.VMEM(*one) for one in out],
        scratch_shapes=[pltpu.VMEM(one.shape, one.dtype) for one in (order, turn, smap)]
        + [pltpu.SemaphoreType.DMA((len(arrays) + 3,))],
        compiler_params=PARAMS,
        name="preload",
    )(*stay(order, turn, smap, *arrays))
    return loaded, table, half_len


def padded(size):
    return -(-size // 128) * 128


def plane_call(received, potential, tables, bands, slots):
    owners = len(received)
    share, grid_side, _ = potential.shape
    width = bands * 2 * slots
    lane_pad = padded(grid_side // 2)
    group = next(g for g in GROUPS if share % g == 0)
    total = owners * slots
    live = total // 2
    return pl.pallas_call(
        functools.partial(
            plane_kernel, sources=owners, bands=bands, slots=slots, share=share, group=group
        ),
        in_specs=[IN_VMEM] * (owners + 5),
        out_shape=[jax.ShapeDtypeStruct((share, width), BF16)] * owners,
        scratch_shapes=[
            pltpu.VMEM((2 * bands * received[0].shape[0], live), F32),
            pltpu.VMEM((live, total), BF16),
            pltpu.VMEM((grid_side // 4, live), F32),
            pltpu.VMEM((live, 2 * lane_pad), BF16),
            pltpu.VMEM((2 * lane_pad, live), BF16),
            pltpu.VMEM((2 * bands * share, live), F32),
        ],
        compiler_params=PARAMS,
        name="planes",
    )(*received, potential, *tables)


def body(coefficients, potential, stick_map, plane_order):
    bands, _, z_span, slots = coefficients.shape
    share, grid_side, _ = potential.shape
    owners = lax.axis_size("fft")
    width = bands * 2 * slots
    rows_sent = -(-(share + 2) // 8) * 8
    me = lax.axis_index("fft").astype(jnp.int32).reshape(1)

    order = plane_order.reshape(1, grid_side)
    turn = z_constants(grid_side, z_span)

    sent = pl.pallas_call(
        functools.partial(stick_kernel, owners=owners, share=share),
        in_specs=[IN_SMEM] + [IN_HBM] * 4,
        out_shape=[jax.ShapeDtypeStruct((rows_sent, width), BF16)] * owners,
        scratch_shapes=[
            pltpu.VMEM(coefficients.shape, BF16),
            pltpu.VMEM(stick_map.shape, jnp.int32),
            pltpu.VMEM(order.shape, jnp.int32),
            pltpu.VMEM(turn.shape, BF16),
            pltpu.VMEM((owners, share, width), BF16),
            pltpu.SemaphoreType.DMA((4,)),
        ],
        compiler_params=PARAMS,
        name="sticks",
    )(me, *stay(coefficients, stick_map, order, turn))

    tables = axis_constants(grid_side, padded(grid_side // 2), padded(grid_side))
    loaded, table, half_len = preload(order, turn, stick_map, [potential, *tables])
    received = exchange(sent, owners, False)

    columns = plane_call(received, loaded[0], loaded[1:], bands, slots)
    returned = exchange(columns, owners, True)
    return pl.pallas_call(
        functools.partial(column_kernel, owners=owners, slots=slots),
        in_specs=[IN_SMEM] + [IN_VMEM] * (owners + 2),
        out_shape=jax.ShapeDtypeStruct(coefficients.shape, F32),
        scratch_shapes=[pltpu.VMEM((owners, share, width), BF16)],
        compiler_params=PARAMS,
        name="columns",
    )(me, half_len, table, *returned)


def solution(mesh):
    placed = (
        P(("groups", "band", "sub"), None, None, "fft"),
        P(("groups", "fft"), None, None),
        P(None, ("groups", "fft")),
        P("groups"),
    )
    return jax.shard_map(
        body,
        mesh=mesh,
        in_specs=placed,
        out_specs=P(("groups", "band", "sub"), None, None, "fft"),
        check_vma=False,
    )
```

```python
import functools
import math

import jax
import jax.numpy as jnp
import numpy as np
from jax import lax
from jax.experimental import pallas as pl
from jax.experimental.pallas import tpu as pltpu
from jax.sharding import PartitionSpec as P

F32 = jnp.float32
BF16 = jnp.bfloat16
PARAMS = pltpu.CompilerParams(vmem_limit_bytes=28 << 20)
IN_SMEM = pl.BlockSpec(memory_space=pltpu.SMEM)
IN_HBM = pl.BlockSpec(memory_space=pltpu.HBM)
IN_VMEM = pl.BlockSpec(memory_space=pltpu.VMEM)
GROUPS = (24, 16, 12, 8, 4, 2)


def stay(*arrays):
    return tuple(pltpu.with_memory_space_constraint(one, pltpu.HBM) for one in arrays)


def angle_tables(left_ids, right_ids, modulus):
    turns = (left_ids[:, None] * right_ids[None, :]) % modulus
    angles = turns * (2.0 * math.pi / modulus)
    return np.cos(angles), np.sin(angles)


def z_constants(grid_side, z_span):
    freq = (np.arange(z_span) - z_span // 2) % grid_side
    return jnp.asarray(np.concatenate(angle_tables(np.arange(grid_side), freq, grid_side), 1), BF16)


def axis_constants(grid_side, lane_pad, pair_pad):
    half = grid_side // 2
    compact = np.arange(half)
    window = np.where(compact < half // 2, compact, compact + half)
    cos_w, sin_w = angle_tables(window, np.arange(grid_side), grid_side)

    def placed(table, phase):
        spare = pair_pad - grid_side
        lanes = (0, spare) if phase == 0 else (spare, 0)
        return np.pad(table, ((0, lane_pad - half), lanes))

    forward_y, inverse_y = [], []
    for phase in range(2):
        cos_p, sin_p = placed(cos_w, phase), placed(sin_w, phase)
        forward_y.append([np.concatenate([cos_p, -sin_p], 0), np.concatenate([sin_p, cos_p], 0)])
        inverse_y.append([np.concatenate([cos_p.T, -sin_p.T], 1), np.concatenate([sin_p.T, cos_p.T], 1)])
    forward_x = np.concatenate(
        [np.concatenate([cos_w.T, -sin_w.T], 1), np.concatenate([sin_w.T, cos_w.T], 1)], 0
    )
    inverse_x = [np.concatenate([cos_w, -sin_w], 0), np.concatenate([sin_w, cos_w], 0)]
    return tuple(jnp.asarray(np.array(t), BF16) for t in (forward_x, forward_y, inverse_y, inverse_x))


def mm(left, right):
    return jnp.dot(left, right, preferred_element_type=F32)


def mm_t(left, right):
    return lax.dot_general(left, right, (((0,), (0,)), ((), ())), preferred_element_type=F32)


def one_hot_columns(ids, count):
    rows = lax.broadcasted_iota(jnp.int32, (count, ids.shape[1]), 0).astype(jnp.int16)
    ids = jnp.broadcast_to(ids, (16, ids.shape[1])).astype(jnp.int16)
    ids = jnp.concatenate([ids] * (count // 16), 0)
    return jnp.where(rows == ids, jnp.ones((), BF16), jnp.zeros((), BF16))


def hops(owners):
    return (0,) + tuple(range(owners - 1, 0, -1))


def partner(index, hop, owners):
    return index ^ hop if owners & (owners - 1) == 0 else (index + hop) % owners


def copies_in(sources, targets, sems):
    started = [
        pltpu.make_async_copy(src, dst, sems.at[i]) for i, (src, dst) in enumerate(zip(sources, targets))
    ]
    for one in started:
        one.start()
    return started


def stick_kernel(me, coeff_h, smap_h, order_h, turn_h, *refs, owners, share):
    outs = refs[:owners]
    coeff, smap, order, turn, sticks, sems = refs[owners:]
    started = copies_in((order_h, turn_h, smap_h, coeff_h), (order, turn, smap, coeff), sems)
    bands, _, z_span, slots = coeff.shape
    grid_side = order.shape[1]
    started[0].wait()
    chosen = one_hot_columns(order[...], grid_side)
    started[1].wait()
    rows = mm_t(chosen, turn[...]).astype(BF16)
    cos_rows, sin_rows = rows[:, :z_span], rows[:, z_span:]
    lefts = (
        jnp.concatenate([cos_rows, -sin_rows], 1),
        jnp.concatenate([sin_rows, cos_rows], 1),
    )
    started[2].wait()
    entries = lax.broadcasted_iota(jnp.int32, (z_span, slots), 0)
    half = (smap[2:3, :] + 1) // 2 - 1
    keep = jnp.abs(entries - z_span // 2) <= half
    started[3].wait()
    for band in range(bands):
        parts = []
        for comp in range(2):
            values = coeff[band, comp].astype(F32)
            parts.append(jnp.where(keep, values, 0.0).astype(BF16))
        masked = jnp.concatenate(parts, 0)
        for comp in range(2):
            found = mm(lefts[comp], masked).astype(BF16)
            col = (band * 2 + comp) * slots
            for owner in range(owners):
                sticks[owner, :, col : col + slots] = found[owner * share : (owner + 1) * share]
    spare = outs[0].shape[0] - share
    live = jnp.where(half >= 0, 1.0, 0.0)
    upper = lax.broadcasted_iota(jnp.int32, (slots, slots), 0)
    upper = upper < lax.broadcasted_iota(jnp.int32, (slots, slots), 1)
    upper = jnp.where(upper, 1.0, 0.0).astype(BF16)
    number = mm(jnp.broadcast_to(live, (8, slots)).astype(BF16), upper)[0:1]
    number = jnp.where(half >= 0, number, -1.0)
    count = jnp.broadcast_to(jnp.sum(live, axis=1, keepdims=True), (1, slots))
    places = jnp.concatenate(
        [
            jnp.concatenate([smap[0:1, :], smap[1:2, :]], 1).astype(F32),
            jnp.concatenate([number, count], 1),
            jnp.zeros((spare - 2, 2 * slots), F32),
        ],
        0,
    ).astype(BF16)
    for out, hop in zip(outs, hops(owners)):
        out[0:share, :] = sticks[partner(me[0], hop, owners)]
        out[share:, 0 : 2 * slots] = places
        if bands > 1:
            out[share:, 2 * slots :] = jnp.zeros((spare, (bands - 1) * 2 * slots), BF16)


def plane_kernel(*refs, sources, bands, slots, share, group):
    recv = refs[:sources]
    pot_h, pot_first, fwd_x, fwd_y, inv_y, inv_x = refs[sources : sources + 6]
    outs = refs[sources + 6 : 2 * sources + 6]
    vals, select, low, high_t, high, acc, pot_later, sems = refs[2 * sources + 6 :]
    grid_side = pot_first.shape[1]
    steps = share // group

    def pot_copy(step):
        rows = pl.ds(step * group, group)
        return pltpu.make_async_copy(pot_h.at[rows], pot_later.at[step - 1], sems.at[step - 1])

    for step in range(1, steps):
        pot_copy(step).start()
    half = grid_side // 2
    quarter = half // 2
    lane_pad = high.shape[0] // 2
    pair_pad = fwd_y.shape[3]
    overlap = 2 * grid_side - pair_pad

    live_count = low.shape[1]
    before = jnp.zeros((1, slots), F32)
    gathered = None
    for src in range(sources):
        cols = slice(src * slots, (src + 1) * slots)
        places = recv[src][share:, :].astype(F32)
        number = places[1:2, 0:slots]
        number = jnp.where(number >= 0.0, number + before, -1.0)
        before = before + places[1:2, slots : 2 * slots]
        chosen = one_hot_columns(number.astype(jnp.int32), live_count)
        select[:, cols] = chosen
        pieces = [recv[src][:, i * slots : (i + 1) * slots] for i in range(2 * bands)]
        part = lax.dot_general(
            jnp.concatenate(pieces, 0), chosen, (((1,), (1,)), ((), ())), preferred_element_type=F32
        )
        gathered = part if gathered is None else gathered + part
    vals[...] = gathered
    rows_sent = recv[0].shape[0]

    def compacted(row):
        ids = row.astype(jnp.int32)
        return jnp.clip(jnp.where(ids < quarter, ids, ids - half), 0, half - 1)

    x_id = compacted(gathered[share : share + 1])
    y_id = compacted(gathered[rows_sent + share : rows_sent + share + 1])
    x_high = jnp.where(x_id >= quarter, 1, 0)
    x_low = x_id - x_high * quarter
    rows = lax.broadcasted_iota(jnp.int32, (quarter, live_count), 0)
    low[...] = jnp.where(rows == x_low, 1.0, 0.0)
    hot = one_hot_columns(x_high * lane_pad + y_id, 2 * lane_pad)
    high[...] = hot
    high_t[...] = hot.T

    def one_group(step):
        base = step * group
        pot = pot_first if step == 0 else pot_later.at[step - 1]
        pairs = [((p, band), (p + 1, band)) for p in range(0, group, 2) for band in range(bands)]
        bundles = [pairs[i : i + 2] for i in range(0, len(pairs), 2)]
        low_hot = low[...].astype(BF16)

        def by_phase(bundle):
            return [[pair[phase] for pair in bundle] for phase in range(2)]

        def spread(units):
            stacked = []
            for plane, band in units:
                for comp in range(2):
                    row = vals[pl.ds((band * 2 + comp) * rows_sent + base + plane, 1), :]
                    stacked.append(jnp.broadcast_to(row, low_hot.shape).astype(BF16) * low_hot)
            spots = mm(jnp.concatenate(stacked, 0), high_t[...]).astype(BF16)
            rows = []
            for i in range(len(units)):
                real = spots[i * half : i * half + quarter]
                imag = spots[i * half + quarter : (i + 1) * half]
                for lanes in (slice(0, lane_pad), slice(lane_pad, 2 * lane_pad)):
                    rows.append(jnp.concatenate([real[:, lanes], imag[:, lanes]], 1))
            return jnp.concatenate(rows, 0)

        def along_y(grids):
            parts = []
            for comp in range(2):
                found = [mm(grid, fwd_y[phase, comp]).astype(BF16) for phase, grid in enumerate(grids)]
                lanes = []
                for i in range(found[0].shape[0] // half):
                    first, second = (one[i * half : (i + 1) * half] for one in found)
                    lanes += [first[:, :overlap], first[:, overlap:] + second[:, :-overlap]]
                    lanes.append(second[:, -overlap:])
                parts.append(jnp.concatenate(lanes, 1))
            return jnp.concatenate(parts, 0)

        def along_x(bundle, grid):
            fields = mm(fwd_x[...], grid)
            field = jnp.concatenate([pot[plane] for pair in bundle for plane, _ in pair], 1)
            return [
                (fields[comp * grid_side : (comp + 1) * grid_side] * field).astype(BF16)
                for comp in range(2)
            ]

        def back_x(product):
            return (mm(inv_x[0], product[0]) + mm(inv_x[1], product[1])).astype(BF16)

        def back_y(grid, count):
            result = []
            for phase in range(2):
                total = None
                for comp in range(2):
                    rows = []
                    for i in range(count):
                        start = i * 2 * grid_side + phase * overlap
                        rows.append(grid[comp * half : (comp + 1) * half, start : start + pair_pad])
                    part = mm(jnp.concatenate(rows, 0), inv_y[phase, comp])
                    total = part if total is None else total + part
                result.append(total.astype(BF16))
            return result

        def pick(units, grid):
            stacked = []
            for i in range(len(units)):
                top = grid[i * half : i * half + quarter]
                bottom = grid[i * half + quarter : (i + 1) * half]
                for lanes in (slice(0, lane_pad), slice(lane_pad, 2 * lane_pad)):
                    stacked.append(jnp.concatenate([top[:, lanes], bottom[:, lanes]], 1))
            found = mm(jnp.concatenate(stacked, 0), high[...])
            for i, (plane, band) in enumerate(units):
                for comp in range(2):
                    start = i * half + comp * quarter
                    line = jnp.sum(found[start : start + quarter] * low[...], axis=0, keepdims=True)
                    acc[pl.ds((band * 2 + comp) * share + base + plane, 1), :] = line

        grids = [[spread(units) for units in by_phase(bundle)] for bundle in bundles]
        grids = [along_y(grid) for grid in grids]
        products = [along_x(bundle, grid) for bundle, grid in zip(bundles, grids)]
        grids = [back_x(product) for product in products]
        grids = [back_y(grid, len(bundle)) for bundle, grid in zip(bundles, grids)]
        for bundle, grid in zip(bundles, grids):
            for units, part in zip(by_phase(bundle), grid):
                pick(units, part)

    for step in range(steps):
        if step > 0:
            pot_copy(step).wait()
        one_group(step)

    spread_out = mm(acc[...].astype(BF16), select[...]).astype(BF16)
    for src in range(sources):
        for i in range(2 * bands):
            outs[src][:, i * slots : (i + 1) * slots] = spread_out[
                i * share : (i + 1) * share, src * slots : (src + 1) * slots
            ]


def column_kernel(me, half_len, table, *refs, owners, slots):
    returned, (out, grid) = refs[:owners], refs[owners:]
    bands, _, z_span, _ = out.shape
    for part, hop in zip(returned, hops(owners)):
        grid[partner(me[0], hop, owners)] = part[...]
    entries = lax.broadcasted_iota(jnp.int32, (z_span, slots), 0)
    keep = jnp.abs(entries - z_span // 2) <= half_len[0:1, :]
    grid_side = table.shape[1]
    scale = jnp.where(keep, 1.0 / grid_side**3, 0.0)
    for band in range(bands):
        lines = []
        for comp in range(2):
            col = (band * 2 + comp) * slots
            lines.append(
                jnp.concatenate([grid[owner, :, col : col + slots] for owner in range(owners)], 0)
            )
        by_real = mm(table[...], lines[0])
        by_imag = mm(table[...], lines[1])
        out[band, 0] = (by_real[:z_span] + by_imag[z_span:]) * scale
        out[band, 1] = (by_imag[:z_span] - by_real[z_span:]) * scale


def exchange(parts, owners, back):
    result = [parts[0]]
    for part, hop in zip(parts[1:], hops(owners)[1:]):
        pairs = [(i, partner(i, hop, owners)) for i in range(owners)]
        if back:
            pairs = [(there, here) for here, there in pairs]
        with jax.named_scope(("back" if back else "send") + str(hop)):
            result.append(lax.ppermute(part, "fft", pairs))
    return result


def preload_kernel(order_h, turn_h, smap_h, *refs):
    count = (len(refs) - 6) // 2
    table, half_len, order, turn, smap, sems = refs[2 * count :]
    wanted = [
        one.at[pl.ds(0, target.shape[0])] if one.shape != target.shape else one
        for one, target in zip(refs[:count], refs[count : 2 * count])
    ]
    started = copies_in(
        (order_h, turn_h, smap_h, *wanted), (order, turn, smap, *refs[count : 2 * count]), sems
    )
    for one in started[:3]:
        one.wait()
    chosen = one_hot_columns(order[...], order.shape[1])
    table[...] = mm_t(turn[...], chosen).astype(BF16)
    half = (smap[2:3, :] + 1) // 2 - 1
    half_len[...] = jnp.broadcast_to(half, half_len.shape)
    for one in started[3:]:
        one.wait()


def preload(order, turn, smap, potential, tables):
    arrays = [potential, *tables]
    out = [((group_size(potential.shape[0]),) + potential.shape[1:], F32)]
    out += [(one.shape, one.dtype) for one in tables]
    out += [((turn.shape[1], order.shape[1]), BF16), ((8, smap.shape[1]), jnp.int32)]
    *loaded, table, half_len = pl.pallas_call(
        preload_kernel,
        in_specs=[IN_HBM] * (len(arrays) + 3),
        out_specs=[IN_VMEM] * len(out),
        out_shape=[pltpu.VMEM(*one) for one in out],
        scratch_shapes=[pltpu.VMEM(one.shape, one.dtype) for one in (order, turn, smap)]
        + [pltpu.SemaphoreType.DMA((len(arrays) + 3,))],
        compiler_params=PARAMS,
        name="preload",
    )(*stay(order, turn, smap, *arrays))
    return loaded, table, half_len


def padded(size):
    return -(-size // 128) * 128


def group_size(share):
    return next(g for g in GROUPS if share % g == 0)


def plane_call(received, potential, pot_first, tables, bands, slots):
    owners = len(received)
    share, grid_side, _ = potential.shape
    width = bands * 2 * slots
    lane_pad = padded(grid_side // 2)
    group = group_size(share)
    later = max(share // group - 1, 1)
    total = owners * slots
    live = total // 2
    return pl.pallas_call(
        functools.partial(
            plane_kernel, sources=owners, bands=bands, slots=slots, share=share, group=group
        ),
        in_specs=[IN_VMEM] * owners + [IN_HBM] + [IN_VMEM] * 5,
        out_shape=[jax.ShapeDtypeStruct((share, width), BF16)] * owners,
        scratch_shapes=[
            pltpu.VMEM((2 * bands * received[0].shape[0], live), F32),
            pltpu.VMEM((live, total), BF16),
            pltpu.VMEM((grid_side // 4, live), F32),
            pltpu.VMEM((live, 2 * lane_pad), BF16),
            pltpu.VMEM((2 * lane_pad, live), BF16),
            pltpu.VMEM((2 * bands * share, live), F32),
            pltpu.VMEM((later, group, grid_side, grid_side), F32),
            pltpu.SemaphoreType.DMA((later,)),
        ],
        compiler_params=PARAMS,
        name="planes",
    )(*received, *stay(potential), pot_first, *tables)


def body(coefficients, potential, stick_map, plane_order):
    bands, _, z_span, slots = coefficients.shape
    share, grid_side, _ = potential.shape
    owners = lax.axis_size("fft")
    width = bands * 2 * slots
    rows_sent = -(-(share + 2) // 8) * 8
    me = lax.axis_index("fft").astype(jnp.int32).reshape(1)

    order = plane_order.reshape(1, grid_side)
    turn = z_constants(grid_side, z_span)

    sent = pl.pallas_call(
        functools.partial(stick_kernel, owners=owners, share=share),
        in_specs=[IN_SMEM] + [IN_HBM] * 4,
        out_shape=[jax.ShapeDtypeStruct((rows_sent, width), BF16)] * owners,
        scratch_shapes=[
            pltpu.VMEM(coefficients.shape, BF16),
            pltpu.VMEM(stick_map.shape, jnp.int32),
            pltpu.VMEM(order.shape, jnp.int32),
            pltpu.VMEM(turn.shape, BF16),
            pltpu.VMEM((owners, share, width), BF16),
            pltpu.SemaphoreType.DMA((4,)),
        ],
        compiler_params=PARAMS,
        name="sticks",
    )(me, *stay(coefficients, stick_map, order, turn))

    tables = axis_constants(grid_side, padded(grid_side // 2), padded(grid_side))
    loaded, table, half_len = preload(order, turn, stick_map, potential, tables)
    received = exchange(sent, owners, False)

    columns = plane_call(received, potential, loaded[0], loaded[1:], bands, slots)
    returned = exchange(columns, owners, True)
    return pl.pallas_call(
        functools.partial(column_kernel, owners=owners, slots=slots),
        in_specs=[IN_SMEM] + [IN_VMEM] * (owners + 2),
        out_shape=jax.ShapeDtypeStruct(coefficients.shape, F32),
        scratch_shapes=[pltpu.VMEM((owners, share, width), BF16)],
        compiler_params=PARAMS,
        name="columns",
    )(me, half_len, table, *returned)


def solution(mesh):
    placed = (
        P(("groups", "band", "sub"), None, None, "fft"),
        P(("groups", "fft"), None, None),
        P(None, ("groups", "fft")),
        P("groups"),
    )
    return jax.shard_map(
        body,
        mesh=mesh,
        in_specs=placed,
        out_specs=P(("groups", "band", "sub"), None, None, "fft"),
        check_vma=False,
    )
```

```python
import functools
import math

import jax
import jax.numpy as jnp
import numpy as np
from jax import lax
from jax.experimental import pallas as pl
from jax.experimental.pallas import tpu as pltpu
from jax.sharding import PartitionSpec as P

F32 = jnp.float32
BF16 = jnp.bfloat16
PARAMS = pltpu.CompilerParams(vmem_limit_bytes=28 << 20)
IN_SMEM = pl.BlockSpec(memory_space=pltpu.SMEM)
PLANE_PARAMS = PARAMS
IN_HBM = pl.BlockSpec(memory_space=pltpu.HBM)
IN_VMEM = pl.BlockSpec(memory_space=pltpu.VMEM)
LAG = 6
TILE = 256
GROUPS = (24, 16, 12, 8, 4, 2)


def stay(*arrays):
    return tuple(pltpu.with_memory_space_constraint(one, pltpu.HBM) for one in arrays)


def angle_tables(left_ids, right_ids, modulus):
    turns = (left_ids[:, None] * right_ids[None, :]) % modulus
    angles = turns * (2.0 * math.pi / modulus)
    return np.cos(angles), np.sin(angles)


def z_constants(grid_side, z_span):
    freq = (np.arange(z_span) - z_span // 2) % grid_side
    return jnp.asarray(np.concatenate(angle_tables(np.arange(grid_side), freq, grid_side), 1), BF16)


def axis_constants(grid_side, lane_pad, pair_pad):
    half = grid_side // 2
    compact = np.arange(half)
    window = np.where(compact < half // 2, compact, compact + half)
    cos_w, sin_w = angle_tables(window, np.arange(grid_side), grid_side)

    def placed(table, phase):
        spare = pair_pad - grid_side
        lanes = (0, spare) if phase == 0 else (spare, 0)
        return np.pad(table, ((0, lane_pad - half), lanes))

    forward_y, inverse_y = [], []
    for phase in range(2):
        cos_p, sin_p = placed(cos_w, phase), placed(sin_w, phase)
        forward_y.append([np.concatenate([cos_p, -sin_p], 0), np.concatenate([sin_p, cos_p], 0)])
        inverse_y.append([np.concatenate([cos_p.T, -sin_p.T], 1), np.concatenate([sin_p.T, cos_p.T], 1)])
    forward_x = np.concatenate(
        [np.concatenate([cos_w.T, -sin_w.T], 1), np.concatenate([sin_w.T, cos_w.T], 1)], 0
    )
    inverse_x = [np.concatenate([cos_w, -sin_w], 0), np.concatenate([sin_w, cos_w], 0)]
    return tuple(jnp.asarray(np.array(t), BF16) for t in (forward_x, forward_y, inverse_y, inverse_x))


def mm(left, right):
    return jnp.dot(left, right, preferred_element_type=F32)


def mm_t(left, right):
    return lax.dot_general(left, right, (((0,), (0,)), ((), ())), preferred_element_type=F32)


def one_hot_columns(ids, count):
    rows = lax.broadcasted_iota(jnp.int32, (count, ids.shape[1]), 0).astype(jnp.int16)
    ids = jnp.broadcast_to(ids, (16, ids.shape[1])).astype(jnp.int16)
    ids = jnp.concatenate([ids] * (count // 16), 0)
    return jnp.where(rows == ids, jnp.ones((), BF16), jnp.zeros((), BF16))


def hops(owners):
    return (0,) + tuple(range(owners - 1, 0, -1))


def partner(index, hop, owners):
    return index ^ hop if owners & (owners - 1) == 0 else (index + hop) % owners


def copies_in(sources, targets, sems):
    started = [
        pltpu.make_async_copy(src, dst, sems.at[i]) for i, (src, dst) in enumerate(zip(sources, targets))
    ]
    for one in started:
        one.start()
    return started


def stick_kernel(me, coeff_h, smap_h, order_h, turn_h, *refs, owners, share):
    outs = refs[:owners]
    coeff, smap, order, turn, sticks, sems = refs[owners:]
    started = copies_in((order_h, turn_h, smap_h, coeff_h), (order, turn, smap, coeff), sems)
    bands, _, z_span, slots = coeff.shape
    grid_side = order.shape[1]
    started[0].wait()
    chosen = one_hot_columns(order[...], grid_side)
    started[1].wait()
    rows = mm_t(chosen, turn[...]).astype(BF16)
    cos_rows, sin_rows = rows[:, :z_span], rows[:, z_span:]
    lefts = (
        jnp.concatenate([cos_rows, -sin_rows], 1),
        jnp.concatenate([sin_rows, cos_rows], 1),
    )
    started[2].wait()
    entries = lax.broadcasted_iota(jnp.int32, (z_span, slots), 0)
    half = (smap[2:3, :] + 1) // 2 - 1
    keep = jnp.abs(entries - z_span // 2) <= half
    started[3].wait()
    for band in range(bands):
        parts = []
        for comp in range(2):
            values = coeff[band, comp].astype(F32)
            parts.append(jnp.where(keep, values, 0.0).astype(BF16))
        masked = jnp.concatenate(parts, 0)
        for comp in range(2):
            found = mm(lefts[comp], masked).astype(BF16)
            col = (band * 2 + comp) * slots
            for owner in range(owners):
                sticks[owner, :, col : col + slots] = found[owner * share : (owner + 1) * share]
    spare = outs[0].shape[0] - share
    live = jnp.where(half >= 0, 1.0, 0.0)
    upper = lax.broadcasted_iota(jnp.int32, (slots, slots), 0)
    upper = upper < lax.broadcasted_iota(jnp.int32, (slots, slots), 1)
    upper = jnp.where(upper, 1.0, 0.0).astype(BF16)
    number = mm(jnp.broadcast_to(live, (8, slots)).astype(BF16), upper)[0:1]
    number = jnp.where(half >= 0, number, -1.0)
    count = jnp.broadcast_to(jnp.sum(live, axis=1, keepdims=True), (1, slots))
    places = jnp.concatenate(
        [
            jnp.concatenate([smap[0:1, :], smap[1:2, :]], 1).astype(F32),
            jnp.concatenate([number, count], 1),
            jnp.zeros((spare - 2, 2 * slots), F32),
        ],
        0,
    ).astype(BF16)
    for out, hop in zip(outs, hops(owners)):
        out[0:share, :] = sticks[partner(me[0], hop, owners)]
        out[share:, 0 : 2 * slots] = places
        if bands > 1:
            out[share:, 2 * slots :] = jnp.zeros((spare, (bands - 1) * 2 * slots), BF16)


def plane_kernel(*refs, sources, bands, slots, share, group):
    recv = refs[:sources]
    pot_h, pot_first, fwd_x, fwd_y, inv_y, inv_x = refs[sources : sources + 6]
    outs = refs[sources + 6 : 2 * sources + 6]
    vals, select, low, high_t, high, acc, pot_later, sems = refs[2 * sources + 6 :]
    grid_side = pot_first.shape[1]
    steps = share // group

    def pot_copy(step):
        rows = pl.ds(step * group, group)
        return pltpu.make_async_copy(pot_h.at[rows], pot_later.at[step - 1], sems.at[step - 1])

    for step in range(1, steps):
        pot_copy(step).start()
    half = grid_side // 2
    quarter = half // 2
    lane_pad = high.shape[0] // 2
    pair_pad = fwd_y.shape[3]
    overlap = 2 * grid_side - pair_pad

    live_count = low.shape[1]
    before = jnp.zeros((1, slots), F32)
    gathered = None
    for src in range(sources):
        cols = slice(src * slots, (src + 1) * slots)
        places = recv[src][share:, :].astype(F32)
        number = places[1:2, 0:slots]
        number = jnp.where(number >= 0.0, number + before, -1.0)
        before = before + places[1:2, slots : 2 * slots]
        chosen = one_hot_columns(number.astype(jnp.int32), live_count)
        select[:, cols] = chosen
        pieces = [recv[src][:, i * slots : (i + 1) * slots] for i in range(2 * bands)]
        part = lax.dot_general(
            jnp.concatenate(pieces, 0), chosen, (((1,), (1,)), ((), ())), preferred_element_type=F32
        )
        gathered = part if gathered is None else gathered + part
    vals[...] = gathered
    rows_sent = recv[0].shape[0]

    def compacted(row):
        ids = row.astype(jnp.int32)
        return jnp.clip(jnp.where(ids < quarter, ids, ids - half), 0, half - 1)

    x_id = compacted(gathered[share : share + 1])
    y_id = compacted(gathered[rows_sent + share : rows_sent + share + 1])
    x_high = jnp.where(x_id >= quarter, 1, 0)
    x_low = x_id - x_high * quarter
    rows = lax.broadcasted_iota(jnp.int32, (quarter, live_count), 0)
    low[...] = jnp.where(rows == x_low, 1.0, 0.0)
    hot = one_hot_columns(x_high * lane_pad + y_id, 2 * lane_pad)
    high[...] = hot
    high_t[...] = hot.T

    def one_group(step):
        base = step * group
        pot = pot_first if step == 0 else pot_later.at[step - 1]
        pairs = [((p, band), (p + 1, band)) for p in range(0, group, 2) for band in range(bands)]
        bundles = [pairs[i : i + 2] for i in range(0, len(pairs), 2)]
        low_hot = low[...].astype(BF16)

        def by_phase(bundle):
            return [[pair[phase] for pair in bundle] for phase in range(2)]

        def spread(units):
            stacked = []
            for plane, band in units:
                for comp in range(2):
                    row = vals[pl.ds((band * 2 + comp) * rows_sent + base + plane, 1), :]
                    stacked.append(jnp.broadcast_to(row, low_hot.shape).astype(BF16) * low_hot)
            spots = mm(jnp.concatenate(stacked, 0), high_t[...]).astype(BF16)
            rows = []
            for i in range(len(units)):
                real = spots[i * half : i * half + quarter]
                imag = spots[i * half + quarter : (i + 1) * half]
                for lanes in (slice(0, lane_pad), slice(lane_pad, 2 * lane_pad)):
                    rows.append(jnp.concatenate([real[:, lanes], imag[:, lanes]], 1))
            return jnp.concatenate(rows, 0)

        def along_y(grids):
            parts = []
            for comp in range(2):
                found = [mm(grid, fwd_y[phase, comp]).astype(BF16) for phase, grid in enumerate(grids)]
                lanes = []
                for i in range(found[0].shape[0] // half):
                    first, second = (one[i * half : (i + 1) * half] for one in found)
                    lanes += [first[:, :overlap], first[:, overlap:] + second[:, :-overlap]]
                    lanes.append(second[:, -overlap:])
                parts.append(jnp.concatenate(lanes, 1))
            return jnp.concatenate(parts, 0)

        def fields_of(bundle):
            return jnp.concatenate([pot[plane] for pair in bundle for plane, _ in pair], 1)

        def along_x(grid, field):
            fields = mm(fwd_x[...], grid)
            return [
                (fields[comp * grid_side : (comp + 1) * grid_side] * field).astype(BF16)
                for comp in range(2)
            ]

        def back_x(product):
            return (mm(inv_x[0], product[0]) + mm(inv_x[1], product[1])).astype(BF16)

        def both_x(bundles, grids):
            tiles = []
            for bundle, grid in zip(bundles, grids):
                field = fields_of(bundle)
                for start in range(0, grid.shape[1], TILE):
                    lanes = slice(start, min(start + TILE, grid.shape[1]))
                    tiles.append((grid[:, lanes], field[:, lanes]))
            products, parts = [], []
            for turn in range(len(tiles) + LAG):
                if turn < len(tiles):
                    products.append(along_x(*tiles[turn]))
                if turn >= LAG:
                    parts.append(back_x(products[turn - LAG]))
            result = []
            for grid in grids:
                count = -(-grid.shape[1] // TILE)
                result.append(jnp.concatenate(parts[:count], 1))
                parts = parts[count:]
            return result

        def back_y(grid, count):
            result = []
            for phase in range(2):
                total = None
                for comp in range(2):
                    rows = []
                    for i in range(count):
                        start = i * 2 * grid_side + phase * overlap
                        rows.append(grid[comp * half : (comp + 1) * half, start : start + pair_pad])
                    part = mm(jnp.concatenate(rows, 0), inv_y[phase, comp])
                    total = part if total is None else total + part
                result.append(total.astype(BF16))
            return result

        def pick(units, grid):
            stacked = []
            for i in range(len(units)):
                top = grid[i * half : i * half + quarter]
                bottom = grid[i * half + quarter : (i + 1) * half]
                for lanes in (slice(0, lane_pad), slice(lane_pad, 2 * lane_pad)):
                    stacked.append(jnp.concatenate([top[:, lanes], bottom[:, lanes]], 1))
            stacked = jnp.concatenate(stacked, 0)
            for start in range(0, high.shape[1], TILE):
                lanes = slice(start, min(start + TILE, high.shape[1]))
                found = mm(stacked, high[:, lanes])
                for i, (plane, band) in enumerate(units):
                    for comp in range(2):
                        top = i * half + comp * quarter
                        line = jnp.sum(found[top : top + quarter] * low[:, lanes], axis=0, keepdims=True)
                        acc[pl.ds((band * 2 + comp) * share + base + plane, 1), lanes] = line

        grids = [[spread(units) for units in by_phase(bundle)] for bundle in bundles]
        grids = [along_y(grid) for grid in grids]
        grids = both_x(bundles, grids)
        grids = [back_y(grid, len(bundle)) for bundle, grid in zip(bundles, grids)]
        for bundle, grid in zip(bundles, grids):
            for units, part in zip(by_phase(bundle), grid):
                pick(units, part)

    for step in range(steps):
        if step > 0:
            pot_copy(step).wait()
        one_group(step)

    spread_out = mm(acc[...].astype(BF16), select[...]).astype(BF16)
    for src in range(sources):
        for i in range(2 * bands):
            outs[src][:, i * slots : (i + 1) * slots] = spread_out[
                i * share : (i + 1) * share, src * slots : (src + 1) * slots
            ]


def column_kernel(me, half_len, table, *refs, owners, slots):
    returned, (out, grid) = refs[:owners], refs[owners:]
    bands, _, z_span, _ = out.shape
    for part, hop in zip(returned, hops(owners)):
        grid[partner(me[0], hop, owners)] = part[...]
    entries = lax.broadcasted_iota(jnp.int32, (z_span, slots), 0)
    keep = jnp.abs(entries - z_span // 2) <= half_len[0:1, :]
    grid_side = table.shape[1]
    scale = jnp.where(keep, 1.0 / grid_side**3, 0.0)
    for band in range(bands):
        lines = []
        for comp in range(2):
            col = (band * 2 + comp) * slots
            lines.append(
                jnp.concatenate([grid[owner, :, col : col + slots] for owner in range(owners)], 0)
            )
        by_real = mm(table[...], lines[0])
        by_imag = mm(table[...], lines[1])
        out[band, 0] = (by_real[:z_span] + by_imag[z_span:]) * scale
        out[band, 1] = (by_imag[:z_span] - by_real[z_span:]) * scale


def exchange(parts, owners, back):
    result = [parts[0]]
    for part, hop in zip(parts[1:], hops(owners)[1:]):
        pairs = [(i, partner(i, hop, owners)) for i in range(owners)]
        if back:
            pairs = [(there, here) for here, there in pairs]
        with jax.named_scope(("back" if back else "send") + str(hop)):
            result.append(lax.ppermute(part, "fft", pairs))
    return result


def preload_kernel(order_h, turn_h, smap_h, *refs):
    count = (len(refs) - 6) // 2
    table, half_len, order, turn, smap, sems = refs[2 * count :]
    wanted = [
        one.at[pl.ds(0, target.shape[0])] if one.shape != target.shape else one
        for one, target in zip(refs[:count], refs[count : 2 * count])
    ]
    started = copies_in(
        (order_h, turn_h, smap_h, *wanted), (order, turn, smap, *refs[count : 2 * count]), sems
    )
    for one in started[:3]:
        one.wait()
    chosen = one_hot_columns(order[...], order.shape[1])
    table[...] = mm_t(turn[...], chosen).astype(BF16)
    half = (smap[2:3, :] + 1) // 2 - 1
    half_len[...] = jnp.broadcast_to(half, half_len.shape)
    for one in started[3:]:
        one.wait()


def preload(order, turn, smap, potential, tables):
    arrays = [potential, *tables]
    out = [((group_size(potential.shape[0]),) + potential.shape[1:], F32)]
    out += [(one.shape, one.dtype) for one in tables]
    out += [((turn.shape[1], order.shape[1]), BF16), ((8, smap.shape[1]), jnp.int32)]
    *loaded, table, half_len = pl.pallas_call(
        preload_kernel,
        in_specs=[IN_HBM] * (len(arrays) + 3),
        out_specs=[IN_VMEM] * len(out),
        out_shape=[pltpu.VMEM(*one) for one in out],
        scratch_shapes=[pltpu.VMEM(one.shape, one.dtype) for one in (order, turn, smap)]
        + [pltpu.SemaphoreType.DMA((len(arrays) + 3,))],
        compiler_params=PARAMS,
        name="preload",
    )(*stay(order, turn, smap, *arrays))
    return loaded, table, half_len


def padded(size):
    return -(-size // 128) * 128


def group_size(share):
    return next(g for g in GROUPS if share % g == 0)


def plane_call(received, potential, pot_first, tables, bands, slots):
    owners = len(received)
    share, grid_side, _ = potential.shape
    width = bands * 2 * slots
    lane_pad = padded(grid_side // 2)
    group = group_size(share)
    later = max(share // group - 1, 1)
    total = owners * slots
    live = total // 2
    return pl.pallas_call(
        functools.partial(
            plane_kernel, sources=owners, bands=bands, slots=slots, share=share, group=group
        ),
        in_specs=[IN_VMEM] * owners + [IN_HBM] + [IN_VMEM] * 5,
        out_shape=[jax.ShapeDtypeStruct((share, width), BF16)] * owners,
        scratch_shapes=[
            pltpu.VMEM((2 * bands * received[0].shape[0], live), F32),
            pltpu.VMEM((live, total), BF16),
            pltpu.VMEM((grid_side // 4, live), F32),
            pltpu.VMEM((live, 2 * lane_pad), BF16),
            pltpu.VMEM((2 * lane_pad, live), BF16),
            pltpu.VMEM((2 * bands * share, live), F32),
            pltpu.VMEM((later, group, grid_side, grid_side), F32),
            pltpu.SemaphoreType.DMA((later,)),
        ],
        compiler_params=PLANE_PARAMS,
        name="planes",
    )(*received, *stay(potential), pot_first, *tables)


def body(coefficients, potential, stick_map, plane_order):
    bands, _, z_span, slots = coefficients.shape
    share, grid_side, _ = potential.shape
    owners = lax.axis_size("fft")
    width = bands * 2 * slots
    rows_sent = -(-(share + 2) // 8) * 8
    me = lax.axis_index("fft").astype(jnp.int32).reshape(1)

    order = plane_order.reshape(1, grid_side)
    turn = z_constants(grid_side, z_span)

    sent = pl.pallas_call(
        functools.partial(stick_kernel, owners=owners, share=share),
        in_specs=[IN_SMEM] + [IN_HBM] * 4,
        out_shape=[jax.ShapeDtypeStruct((rows_sent, width), BF16)] * owners,
        scratch_shapes=[
            pltpu.VMEM(coefficients.shape, BF16),
            pltpu.VMEM(stick_map.shape, jnp.int32),
            pltpu.VMEM(order.shape, jnp.int32),
            pltpu.VMEM(turn.shape, BF16),
            pltpu.VMEM((owners, share, width), BF16),
            pltpu.SemaphoreType.DMA((4,)),
        ],
        compiler_params=PARAMS,
        name="sticks",
    )(me, *stay(coefficients, stick_map, order, turn))

    tables = axis_constants(grid_side, padded(grid_side // 2), padded(grid_side))
    loaded, table, half_len = preload(order, turn, stick_map, potential, tables)
    received = exchange(sent, owners, False)

    columns = plane_call(received, potential, loaded[0], loaded[1:], bands, slots)
    returned = exchange(columns, owners, True)
    return pl.pallas_call(
        functools.partial(column_kernel, owners=owners, slots=slots),
        in_specs=[IN_SMEM] + [IN_VMEM] * (owners + 2),
        out_shape=jax.ShapeDtypeStruct(coefficients.shape, F32),
        scratch_shapes=[pltpu.VMEM((owners, share, width), BF16)],
        compiler_params=PARAMS,
        name="columns",
    )(me, half_len, table, *returned)


def solution(mesh):
    placed = (
        P(("groups", "band", "sub"), None, None, "fft"),
        P(("groups", "fft"), None, None),
        P(None, ("groups", "fft")),
        P("groups"),
    )
    return jax.shard_map(
        body,
        mesh=mesh,
        in_specs=placed,
        out_specs=P(("groups", "band", "sub"), None, None, "fft"),
        check_vma=False,
    )
```

```python
import functools
import math

import jax
import jax.numpy as jnp
import numpy as np
from jax import lax
from jax.experimental import pallas as pl
from jax.experimental.pallas import tpu as pltpu
from jax.sharding import PartitionSpec as P

F32 = jnp.float32
BF16 = jnp.bfloat16
PARAMS = pltpu.CompilerParams(vmem_limit_bytes=28 << 20)
IN_SMEM = pl.BlockSpec(memory_space=pltpu.SMEM)
PLANE_PARAMS = PARAMS
IN_HBM = pl.BlockSpec(memory_space=pltpu.HBM)
IN_VMEM = pl.BlockSpec(memory_space=pltpu.VMEM)
LAG = 6
TILE = 256
GROUPS = (24, 16, 12, 8, 4, 2)


def stay(*arrays):
    return tuple(pltpu.with_memory_space_constraint(one, pltpu.HBM) for one in arrays)


def angle_tables(left_ids, right_ids, modulus):
    turns = (left_ids[:, None] * right_ids[None, :]) % modulus
    angles = turns * (2.0 * math.pi / modulus)
    return np.cos(angles), np.sin(angles)


def z_constants(grid_side, z_span):
    freq = (np.arange(z_span) - z_span // 2) % grid_side
    return jnp.asarray(np.concatenate(angle_tables(np.arange(grid_side), freq, grid_side), 1), BF16)


def axis_constants(grid_side, lane_pad, pair_pad):
    half = grid_side // 2
    compact = np.arange(half)
    window = np.where(compact < half // 2, compact, compact + half)
    cos_w, sin_w = angle_tables(window, np.arange(grid_side), grid_side)

    def placed(table, phase):
        spare = pair_pad - grid_side
        lanes = (0, spare) if phase == 0 else (spare, 0)
        return np.pad(table, ((0, lane_pad - half), lanes))

    forward_y, inverse_y = [], []
    for phase in range(2):
        cos_p, sin_p = placed(cos_w, phase), placed(sin_w, phase)
        forward_y.append([np.concatenate([cos_p, -sin_p], 0), np.concatenate([sin_p, cos_p], 0)])
        inverse_y.append([np.concatenate([cos_p.T, -sin_p.T], 1), np.concatenate([sin_p.T, cos_p.T], 1)])
    forward_x = np.concatenate(
        [np.concatenate([cos_w.T, -sin_w.T], 1), np.concatenate([sin_w.T, cos_w.T], 1)], 0
    )
    inverse_x = [np.concatenate([cos_w, -sin_w], 0), np.concatenate([sin_w, cos_w], 0)]
    return tuple(jnp.asarray(np.array(t), BF16) for t in (forward_x, forward_y, inverse_y, inverse_x))


def mm(left, right):
    return jnp.dot(left, right, preferred_element_type=F32)


def mm_t(left, right):
    return lax.dot_general(left, right, (((0,), (0,)), ((), ())), preferred_element_type=F32)


def one_hot_columns(ids, count):
    rows = lax.broadcasted_iota(jnp.int32, (count, ids.shape[1]), 0).astype(jnp.int16)
    ids = jnp.broadcast_to(ids, (16, ids.shape[1])).astype(jnp.int16)
    ids = jnp.concatenate([ids] * (count // 16), 0)
    return jnp.where(rows == ids, jnp.ones((), BF16), jnp.zeros((), BF16))


def hops(owners):
    return (0,) + tuple(range(owners - 1, 0, -1))


def partner(index, hop, owners):
    return index ^ hop if owners & (owners - 1) == 0 else (index + hop) % owners


def copies_in(sources, targets, sems):
    started = [
        pltpu.make_async_copy(src, dst, sems.at[i]) for i, (src, dst) in enumerate(zip(sources, targets))
    ]
    for one in started:
        one.start()
    return started


def stick_kernel(me, coeff_h, smap_h, order_h, turn_h, *refs, owners, share):
    outs = refs[:owners]
    coeff, smap, order, turn, sticks, sems = refs[owners:]
    started = copies_in((order_h, turn_h, smap_h, coeff_h), (order, turn, smap, coeff), sems)
    bands, _, z_span, slots = coeff.shape
    grid_side = order.shape[1]
    started[0].wait()
    chosen = one_hot_columns(order[...], grid_side)
    started[1].wait()
    rows = mm_t(chosen, turn[...]).astype(BF16)
    cos_rows, sin_rows = rows[:, :z_span], rows[:, z_span:]
    lefts = (
        jnp.concatenate([cos_rows, -sin_rows], 1),
        jnp.concatenate([sin_rows, cos_rows], 1),
    )
    started[2].wait()
    entries = lax.broadcasted_iota(jnp.int32, (z_span, slots), 0)
    half = (smap[2:3, :] + 1) // 2 - 1
    keep = jnp.abs(entries - z_span // 2) <= half
    started[3].wait()
    for band in range(bands):
        parts = []
        for comp in range(2):
            values = coeff[band, comp].astype(F32)
            parts.append(jnp.where(keep, values, 0.0).astype(BF16))
        masked = jnp.concatenate(parts, 0)
        for comp in range(2):
            found = mm(lefts[comp], masked).astype(BF16)
            col = (band * 2 + comp) * slots
            for owner in range(owners):
                sticks[owner, :, col : col + slots] = found[owner * share : (owner + 1) * share]
    spare = outs[0].shape[0] - share
    live = jnp.where(half >= 0, 1.0, 0.0)
    upper = lax.broadcasted_iota(jnp.int32, (slots, slots), 0)
    upper = upper < lax.broadcasted_iota(jnp.int32, (slots, slots), 1)
    upper = jnp.where(upper, 1.0, 0.0).astype(BF16)
    number = mm(jnp.broadcast_to(live, (8, slots)).astype(BF16), upper)[0:1]
    number = jnp.where(half >= 0, number, -1.0)
    count = jnp.broadcast_to(jnp.sum(live, axis=1, keepdims=True), (1, slots))
    places = jnp.concatenate(
        [
            jnp.concatenate([smap[0:1, :], smap[1:2, :]], 1).astype(F32),
            jnp.concatenate([number, count], 1),
            jnp.zeros((spare - 2, 2 * slots), F32),
        ],
        0,
    ).astype(BF16)
    for out, hop in zip(outs, hops(owners)):
        out[0:share, :] = sticks[partner(me[0], hop, owners)]
        out[share:, 0 : 2 * slots] = places
        if bands > 1:
            out[share:, 2 * slots :] = jnp.zeros((spare, (bands - 1) * 2 * slots), BF16)


def plane_kernel(*refs, sources, bands, slots, share, group):
    recv = refs[:sources]
    pot_h, pot_first, fwd_x, fwd_y, inv_y, inv_x = refs[sources : sources + 6]
    outs = refs[sources + 6 : 2 * sources + 6]
    vals, select, low, high_t, high, acc, pot_later, sems = refs[2 * sources + 6 :]
    grid_side = pot_first.shape[1]
    steps = share // group

    def pot_copy(step):
        rows = pl.ds(step * group, group)
        return pltpu.make_async_copy(pot_h.at[rows], pot_later.at[step - 1], sems.at[step - 1])

    for step in range(1, steps):
        pot_copy(step).start()
    half = grid_side // 2
    quarter = half // 2
    lane_pad = high.shape[0] // 2
    pair_pad = fwd_y.shape[3]
    overlap = 2 * grid_side - pair_pad

    live_count = low.shape[1]
    before = jnp.zeros((1, slots), F32)
    gathered = None
    for src in range(sources):
        cols = slice(src * slots, (src + 1) * slots)
        places = recv[src][share:, :].astype(F32)
        number = places[1:2, 0:slots]
        number = jnp.where(number >= 0.0, number + before, -1.0)
        before = before + places[1:2, slots : 2 * slots]
        chosen = one_hot_columns(number.astype(jnp.int32), live_count)
        select[:, cols] = chosen
        pieces = [recv[src][:, i * slots : (i + 1) * slots] for i in range(2 * bands)]
        part = lax.dot_general(
            jnp.concatenate(pieces, 0), chosen, (((1,), (1,)), ((), ())), preferred_element_type=F32
        )
        gathered = part if gathered is None else gathered + part
    vals[...] = gathered
    rows_sent = recv[0].shape[0]

    def compacted(row):
        ids = row.astype(jnp.int32)
        return jnp.clip(jnp.where(ids < quarter, ids, ids - half), 0, half - 1)

    x_id = compacted(gathered[share : share + 1])
    y_id = compacted(gathered[rows_sent + share : rows_sent + share + 1])
    x_high = jnp.where(x_id >= quarter, 1, 0)
    x_low = x_id - x_high * quarter
    rows = lax.broadcasted_iota(jnp.int32, (quarter, live_count), 0)
    low[...] = jnp.where(rows == x_low, 1.0, 0.0)
    hot = one_hot_columns(x_high * lane_pad + y_id, 2 * lane_pad)
    high[...] = hot
    high_t[...] = hot.T

    def one_group(step):
        base = step * group
        pot = pot_first if step == 0 else pot_later.at[step - 1]
        pairs = [((p, band), (p + 1, band)) for p in range(0, group, 2) for band in range(bands)]
        bundles = [pairs[i : i + 2] for i in range(0, len(pairs), 2)]
        low_hot = low[...].astype(BF16)

        def by_phase(bundle):
            return [[pair[phase] for pair in bundle] for phase in range(2)]

        def spread(units):
            stacked = []
            for plane, band in units:
                for comp in range(2):
                    row = vals[pl.ds((band * 2 + comp) * rows_sent + base + plane, 1), :]
                    stacked.append(jnp.broadcast_to(row, low_hot.shape).astype(BF16) * low_hot)
            spots = mm(jnp.concatenate(stacked, 0), high_t[...]).astype(BF16)
            rows = []
            for i in range(len(units)):
                real = spots[i * half : i * half + quarter]
                imag = spots[i * half + quarter : (i + 1) * half]
                for lanes in (slice(0, lane_pad), slice(lane_pad, 2 * lane_pad)):
                    rows.append(jnp.concatenate([real[:, lanes], imag[:, lanes]], 1))
            return jnp.concatenate(rows, 0)

        def along_y(grids):
            parts = []
            for comp in range(2):
                found = [mm(grid, fwd_y[phase, comp]).astype(BF16) for phase, grid in enumerate(grids)]
                lanes = []
                for i in range(found[0].shape[0] // half):
                    first, second = (one[i * half : (i + 1) * half] for one in found)
                    lanes += [first[:, :overlap], first[:, overlap:] + second[:, :-overlap]]
                    lanes.append(second[:, -overlap:])
                parts.append(jnp.concatenate(lanes, 1))
            return jnp.concatenate(parts, 0)

        def fields_of(bundle):
            return jnp.concatenate([pot[plane] for pair in bundle for plane, _ in pair], 1)

        def along_x(grid, field):
            fields = mm(fwd_x[...], grid)
            return [
                (fields[comp * grid_side : (comp + 1) * grid_side] * field).astype(BF16)
                for comp in range(2)
            ]

        def back_x(product):
            return (mm(inv_x[0], product[0]) + mm(inv_x[1], product[1])).astype(BF16)

        def both_x(bundles, grids):
            tiles = []
            for bundle, grid in zip(bundles, grids):
                field = fields_of(bundle)
                for start in range(0, grid.shape[1], TILE):
                    lanes = slice(start, min(start + TILE, grid.shape[1]))
                    tiles.append((grid[:, lanes], field[:, lanes]))
            products, parts = [], []
            for turn in range(len(tiles) + LAG):
                if turn < len(tiles):
                    products.append(along_x(*tiles[turn]))
                if turn >= LAG:
                    parts.append(back_x(products[turn - LAG]))
            result = []
            for grid in grids:
                count = -(-grid.shape[1] // TILE)
                result.append(jnp.concatenate(parts[:count], 1))
                parts = parts[count:]
            return result

        def back_y(grid, count):
            result = []
            for phase in range(2):
                total = None
                for comp in range(2):
                    rows = []
                    for i in range(count):
                        start = i * 2 * grid_side + phase * overlap
                        rows.append(grid[comp * half : (comp + 1) * half, start : start + pair_pad])
                    part = mm(jnp.concatenate(rows, 0), inv_y[phase, comp])
                    total = part if total is None else total + part
                result.append(total.astype(BF16))
            return result

        def pick(units, grid):
            stacked = []
            for i in range(len(units)):
                top = grid[i * half : i * half + quarter]
                bottom = grid[i * half + quarter : (i + 1) * half]
                for lanes in (slice(0, lane_pad), slice(lane_pad, 2 * lane_pad)):
                    stacked.append(jnp.concatenate([top[:, lanes], bottom[:, lanes]], 1))
            stacked = jnp.concatenate(stacked, 0)
            for start in range(0, high.shape[1], TILE):
                lanes = slice(start, min(start + TILE, high.shape[1]))
                found = mm(stacked, high[:, lanes])
                for i, (plane, band) in enumerate(units):
                    for comp in range(2):
                        top = i * half + comp * quarter
                        line = jnp.sum(found[top : top + quarter] * low[:, lanes], axis=0, keepdims=True)
                        acc[pl.ds((band * 2 + comp) * share + base + plane, 1), lanes] = line

        grids = [[spread(units) for units in by_phase(bundle)] for bundle in bundles]
        grids = [along_y(grid) for grid in grids]
        yield
        grids = both_x(bundles, grids)
        grids = [back_y(grid, len(bundle)) for bundle, grid in zip(bundles, grids)]
        yield
        for bundle, grid in zip(bundles, grids):
            for units, part in zip(by_phase(bundle), grid):
                pick(units, part)
        yield

    groups = [one_group(step) for step in range(steps)]
    next(groups[0])
    for step in range(steps):
        if step > 0:
            pot_copy(step).wait()
        next(groups[step])
        if step + 1 < steps:
            next(groups[step + 1])
        next(groups[step])

    spread_out = mm(acc[...].astype(BF16), select[...]).astype(BF16)
    for src in range(sources):
        for i in range(2 * bands):
            outs[src][:, i * slots : (i + 1) * slots] = spread_out[
                i * share : (i + 1) * share, src * slots : (src + 1) * slots
            ]


def column_kernel(me, half_len, table, *refs, owners, slots):
    returned, (out, grid) = refs[:owners], refs[owners:]
    bands, _, z_span, _ = out.shape
    for part, hop in zip(returned, hops(owners)):
        grid[partner(me[0], hop, owners)] = part[...]
    entries = lax.broadcasted_iota(jnp.int32, (z_span, slots), 0)
    keep = jnp.abs(entries - z_span // 2) <= half_len[0:1, :]
    grid_side = table.shape[1]
    scale = jnp.where(keep, 1.0 / grid_side**3, 0.0)
    for band in range(bands):
        lines = []
        for comp in range(2):
            col = (band * 2 + comp) * slots
            lines.append(
                jnp.concatenate([grid[owner, :, col : col + slots] for owner in range(owners)], 0)
            )
        by_real = mm(table[...], lines[0])
        by_imag = mm(table[...], lines[1])
        out[band, 0] = (by_real[:z_span] + by_imag[z_span:]) * scale
        out[band, 1] = (by_imag[:z_span] - by_real[z_span:]) * scale


def exchange(parts, owners, back):
    result = [parts[0]]
    for part, hop in zip(parts[1:], hops(owners)[1:]):
        pairs = [(i, partner(i, hop, owners)) for i in range(owners)]
        if back:
            pairs = [(there, here) for here, there in pairs]
        with jax.named_scope(("back" if back else "send") + str(hop)):
            result.append(lax.ppermute(part, "fft", pairs))
    return result


def preload_kernel(order_h, turn_h, smap_h, *refs):
    count = (len(refs) - 6) // 2
    table, half_len, order, turn, smap, sems = refs[2 * count :]
    wanted = [
        one.at[pl.ds(0, target.shape[0])] if one.shape != target.shape else one
        for one, target in zip(refs[:count], refs[count : 2 * count])
    ]
    started = copies_in(
        (order_h, turn_h, smap_h, *wanted), (order, turn, smap, *refs[count : 2 * count]), sems
    )
    for one in started[:3]:
        one.wait()
    chosen = one_hot_columns(order[...], order.shape[1])
    table[...] = mm_t(turn[...], chosen).astype(BF16)
    half = (smap[2:3, :] + 1) // 2 - 1
    half_len[...] = jnp.broadcast_to(half, half_len.shape)
    for one in started[3:]:
        one.wait()


def preload(order, turn, smap, potential, tables):
    arrays = [potential, *tables]
    out = [((group_size(potential.shape[0]),) + potential.shape[1:], F32)]
    out += [(one.shape, one.dtype) for one in tables]
    out += [((turn.shape[1], order.shape[1]), BF16), ((8, smap.shape[1]), jnp.int32)]
    *loaded, table, half_len = pl.pallas_call(
        preload_kernel,
        in_specs=[IN_HBM] * (len(arrays) + 3),
        out_specs=[IN_VMEM] * len(out),
        out_shape=[pltpu.VMEM(*one) for one in out],
        scratch_shapes=[pltpu.VMEM(one.shape, one.dtype) for one in (order, turn, smap)]
        + [pltpu.SemaphoreType.DMA((len(arrays) + 3,))],
        compiler_params=PARAMS,
        name="preload",
    )(*stay(order, turn, smap, *arrays))
    return loaded, table, half_len


def padded(size):
    return -(-size // 128) * 128


def group_size(share):
    return next(g for g in GROUPS if share % g == 0)


def plane_call(received, potential, pot_first, tables, bands, slots):
    owners = len(received)
    share, grid_side, _ = potential.shape
    width = bands * 2 * slots
    lane_pad = padded(grid_side // 2)
    group = group_size(share)
    later = max(share // group - 1, 1)
    total = owners * slots
    live = total // 2
    return pl.pallas_call(
        functools.partial(
            plane_kernel, sources=owners, bands=bands, slots=slots, share=share, group=group
        ),
        in_specs=[IN_VMEM] * owners + [IN_HBM] + [IN_VMEM] * 5,
        out_shape=[jax.ShapeDtypeStruct((share, width), BF16)] * owners,
        scratch_shapes=[
            pltpu.VMEM((2 * bands * received[0].shape[0], live), F32),
            pltpu.VMEM((live, total), BF16),
            pltpu.VMEM((grid_side // 4, live), F32),
            pltpu.VMEM((live, 2 * lane_pad), BF16),
            pltpu.VMEM((2 * lane_pad, live), BF16),
            pltpu.VMEM((2 * bands * share, live), F32),
            pltpu.VMEM((later, group, grid_side, grid_side), F32),
            pltpu.SemaphoreType.DMA((later,)),
        ],
        compiler_params=PLANE_PARAMS,
        name="planes",
    )(*received, *stay(potential), pot_first, *tables)


def body(coefficients, potential, stick_map, plane_order):
    bands, _, z_span, slots = coefficients.shape
    share, grid_side, _ = potential.shape
    owners = lax.axis_size("fft")
    width = bands * 2 * slots
    rows_sent = -(-(share + 2) // 8) * 8
    me = lax.axis_index("fft").astype(jnp.int32).reshape(1)

    order = plane_order.reshape(1, grid_side)
    turn = z_constants(grid_side, z_span)

    sent = pl.pallas_call(
        functools.partial(stick_kernel, owners=owners, share=share),
        in_specs=[IN_SMEM] + [IN_HBM] * 4,
        out_shape=[jax.ShapeDtypeStruct((rows_sent, width), BF16)] * owners,
        scratch_shapes=[
            pltpu.VMEM(coefficients.shape, BF16),
            pltpu.VMEM(stick_map.shape, jnp.int32),
            pltpu.VMEM(order.shape, jnp.int32),
            pltpu.VMEM(turn.shape, BF16),
            pltpu.VMEM((owners, share, width), BF16),
            pltpu.SemaphoreType.DMA((4,)),
        ],
        compiler_params=PARAMS,
        name="sticks",
    )(me, *stay(coefficients, stick_map, order, turn))

    tables = axis_constants(grid_side, padded(grid_side // 2), padded(grid_side))
    loaded, table, half_len = preload(order, turn, stick_map, potential, tables)
    received = exchange(sent, owners, False)

    columns = plane_call(received, potential, loaded[0], loaded[1:], bands, slots)
    returned = exchange(columns, owners, True)
    return pl.pallas_call(
        functools.partial(column_kernel, owners=owners, slots=slots),
        in_specs=[IN_SMEM] + [IN_VMEM] * (owners + 2),
        out_shape=jax.ShapeDtypeStruct(coefficients.shape, F32),
        scratch_shapes=[pltpu.VMEM((owners, share, width), BF16)],
        compiler_params=PARAMS,
        name="columns",
    )(me, half_len, table, *returned)


def solution(mesh):
    placed = (
        P(("groups", "band", "sub"), None, None, "fft"),
        P(("groups", "fft"), None, None),
        P(None, ("groups", "fft")),
        P("groups"),
    )
    return jax.shard_map(
        body,
        mesh=mesh,
        in_specs=placed,
        out_specs=P(("groups", "band", "sub"), None, None, "fft"),
        check_vma=False,
    )
```
